32 devices in a mesh: dom: 32 (over z, y, x, core).
Axes of the slice: x: 2, y: 2, z: 4, core: 2. Of those that a mesh axis runs over, the one named last changes fastest.
Arguments:
- features: bfloat16 [32768, 512], P('dom'), may hold values from -6 to 6
- embeddings: bfloat16 [32768, 128], P('dom'), may hold values from -6 to 6
- tile_values: bfloat16 [256, 4, 128, 128], P('dom'), may hold values from -4 to 4
- tile_columns: int32 [256, 4], P('dom'), may hold values from 0 to 11
- send_blocks: int32 [32, 2, 2], P('dom'), may hold values from 0 to 7
- send_count: int32 [32, 2], P('dom'), may hold values from 1 to 2, as said below
- hub_rows: int32 [64], P('dom'), may hold values from 0 to 1023, as said below
- hub_weight: bfloat16 [32768, 64], P('dom'), may hold values from -4 to 4
- degree: int32 [32768], P('dom'), may hold values from 16 to 64
Outputs:
- hop_features: bfloat16 [3, 32768, 512], P(None, 'dom')
- hop_embeddings: bfloat16 [3, 32768, 128], P(None, 'dom')
The draws below stay inside these ranges and needn't reach their ends.
Inputs may be any that keep to these rules, and one draw needn't show every extreme that they name: `send_count`: some partition sends 2 blocks to its right and some to its left. `hub_rows`: the 2 hub rows of each partition are distinct local row numbers.
All inputs are finite; a program needn't handle non-finite values.
Results may differ from the reference program's by a relative error of at most 0.012.
Values may be sent and summed in bfloat16 or wider, within the bound.
A program may use at most 64 MiB of HBM per device.

```python
import jax
import jax.numpy as jnp
from jax import lax

F = 512
E = 128
TILE = 128
ROWS_DEV = 1024
K = 4
SEND_MOST = 2
HUB_DEV = 2
HOPS = 3
ROWS = 32768
BLOCKS = 256
HUBS = 64
N_DOM = 32


def draw_send_count(key, part):
    counts = jax.random.randint(key, (N_DOM, 2), 1, SEND_MOST + 1)
    counts = counts.at[0, 1].set(SEND_MOST)
    counts = counts.at[N_DOM - 1, 0].set(SEND_MOST)
    return counts.astype(jnp.int32)


def draw_hub_rows(key, part):

    def one_device(device_index):
        return jax.random.permutation(jax.random.fold_in(key, device_index), ROWS_DEV)[:HUB_DEV]
    chosen = jax.vmap(one_device)(jnp.arange(N_DOM, dtype=jnp.int32))
    return chosen.reshape(-1).astype(jnp.int32)


def plant(array, stream_key, least, high):
    spot = [jax.random.randint(jax.random.fold_in(stream_key, axis), (), 0, length) for axis, length in enumerate(array.shape)]
    longest = array.shape.index(max(array.shape))
    next_to = spot[:longest] + [(spot[longest] + 1) % array.shape[longest]] + spot[longest + 1:]
    return array.at[tuple(spot)].set(least).at[tuple(next_to)].set(high)


def block_scale(own_key, shape, cuts, low, top_value):
    def one(dim, blocks):
        steps = jax.random.uniform(jax.random.fold_in(jax.random.fold_in(own_key, 6), dim), (blocks,), jnp.float32, low / len(cuts), top_value / len(cuts))
        return jnp.repeat(jnp.exp(steps), shape[dim] // blocks).reshape((-1,) + (1,) * (len(shape) - dim - 1))

    level = one(*cuts[0])
    for cut in cuts[1:]:
        level = level * one(*cut)
    return level


def scatter_about(rng, dims, spread, reach, pieces=(), kind=jnp.bfloat16):
    values = spread * jax.random.normal(rng, dims, jnp.float32)
    if pieces:
        values = values * block_scale(rng, dims, pieces, -0.22, 0.18)
    return jnp.clip(values, -reach, reach).astype(kind)


def setup_inputs(seed: int = 0) -> dict:
    key_of = jax.random.split(jax.random.key(seed), 10)
    features = scatter_about(key_of[0], (ROWS, F), 1.0, 6.0, ((0, 32),))
    embeddings = scatter_about(key_of[1], (ROWS, E), 1.0, 6.0, ((0, 32),))
    tile_values = scatter_about(key_of[2], (BLOCKS, K, TILE, TILE), 1.0, 4.0, ((0, 32),))
    tile_columns = plant(jax.random.randint(key_of[3], (BLOCKS, K), 0, ROWS_DEV // TILE + 2 * SEND_MOST), jax.random.fold_in(key_of[3], 1), 0, (ROWS_DEV // TILE + 2 * SEND_MOST) - 1).astype(jnp.int32)
    send_blocks = plant(jax.random.randint(key_of[4], (N_DOM, 2, SEND_MOST), 0, ROWS_DEV // TILE), jax.random.fold_in(key_of[4], 1), 0, (ROWS_DEV // TILE) - 1).astype(jnp.int32)
    send_count = draw_send_count(jax.random.fold_in(key_of[9], 71), 0)
    hub_rows = draw_hub_rows(jax.random.fold_in(key_of[9], 71), 0)
    hub_weight = scatter_about(key_of[7], (ROWS, HUBS), 1.0, 4.0, ((0, 32),))
    degree = plant(jax.random.randint(key_of[8], (ROWS,), 16, 65), jax.random.fold_in(key_of[8], 1), 16, 64).astype(jnp.int32)
    return {"features": features, "embeddings": embeddings, "tile_values": tile_values, "tile_columns": tile_columns, "send_blocks": send_blocks, "send_count": send_count, "hub_rows": hub_rows, "hub_weight": hub_weight, "degree": degree}


def reference(features, embeddings, tile_values, tile_columns, send_blocks, send_count, hub_rows, hub_weight, degree):
    feature_width = F + E
    block_count = ROWS_DEV // TILE
    device_count = N_DOM
    inverse_root = lax.rsqrt(degree.astype(jnp.float32)).reshape(device_count, ROWS_DEV, 1)
    current = jnp.concatenate([features, embeddings], axis=1).reshape(device_count, ROWS_DEV, feature_width)
    tiles_split = tile_values.reshape(device_count, block_count, K, TILE, TILE)
    columns_split = tile_columns.reshape(device_count, block_count, K).astype(jnp.int32)
    hubs_split = hub_rows.reshape(device_count, HUB_DEV).astype(jnp.int32)
    weight_split = hub_weight.reshape(device_count, ROWS_DEV, HUBS)
    live_slots = jnp.arange(SEND_MOST, dtype=jnp.int32)[None, None, :] < send_count[:, :, None]
    empty_rim = jnp.zeros((1, SEND_MOST, TILE, feature_width), jnp.bfloat16)
    results = []
    for hop_index in range(HOPS):
        scaled = (current.astype(jnp.float32) * inverse_root).astype(jnp.bfloat16)
        blocked = scaled.reshape(device_count, block_count, TILE, feature_width)
        outgoing = jax.vmap(lambda source, listed: source[listed])(blocked, send_blocks.astype(jnp.int32))
        outgoing = jnp.where(live_slots[:, :, :, None, None], outgoing, jnp.zeros_like(outgoing))
        from_left = jnp.concatenate([empty_rim, outgoing[:-1, 1]], axis=0)
        from_right = jnp.concatenate([outgoing[1:, 0], empty_rim], axis=0)
        extended = jnp.concatenate([blocked, from_left, from_right], axis=1)
        gathered_hubs = jax.vmap(lambda source, listed: source[listed])(scaled, hubs_split).reshape(HUBS, feature_width)

        def one_device(operands):
            buffer, tiles_here, columns_here, weight_here = operands
            picked = buffer[columns_here]
            local_part = jnp.einsum('bkij,bkjw->biw', tiles_here.astype(jnp.float32), picked.astype(jnp.float32))
            local_part = local_part.reshape(ROWS_DEV, feature_width)
            return local_part + jnp.dot(weight_here, gathered_hubs, preferred_element_type=jnp.float32)
        summed = lax.map(one_device, (extended, tiles_split, columns_split, weight_split))
        current = (summed * inverse_root).astype(jnp.bfloat16)
        results.append(current.reshape(ROWS, feature_width))
    stacked = jnp.stack(results)
    return (stacked[:, :, :F], stacked[:, :, F:])
```

```python
import functools

import jax
import jax.numpy as jnp
from jax import lax
from jax.experimental import pallas as pl
from jax.experimental.pallas import tpu as pltpu
from jax.sharding import PartitionSpec as P

HOPS = 3
LANES = 128
WIDTH = 256
UNROLL = 4
VMEM = 67043328
MESH = pl.DeviceIdType.MESH


def cut(which, columns):
    return [(which, at, min(WIDTH, columns - at)) for at in range(0, columns, WIDTH)]


def kernel(
    n, sizes, cols_hbm, listed_hbm, count_hbm, hubs_hbm,
    features_hbm, embeddings_hbm, tiles_hbm, weight_hbm, degree_hbm,
    out_f, out_e, *scratch,
):
    blocks, tile, taps, send_most, hub_dev, pieces, plane = sizes
    planes = n // plane
    chunks = len(pieces)
    per = tile // 16
    pairs = HOPS * chunks
    scratch = list(scratch)
    take = lambda count: [scratch.pop(0) for _ in range(count)]
    locals_, groups, exts, sends, hub_sends, hub_bufs = (take(pairs) for _ in range(6))
    (
        cols_ref, listed_ref, count_ref, hubs_ref,
        features, embeddings, tiles, weight_t, degree, weight, inv,
        load_sem, rim_send_sem, rim_recv_sem, hub_send_sem, hub_recv_sem, ready,
    ) = scratch
    me = lax.axis_index("dom")

    loads = [
        pltpu.make_async_copy(source, held, load_sem.at[q])
        for q, (source, held) in enumerate(
            (
                (degree_hbm, degree),
                (features_hbm, features),
                (embeddings_hbm, embeddings),
                (tiles_hbm, tiles),
                (weight_hbm, weight_t),
                (cols_hbm, cols_ref),
                (listed_hbm, listed_ref),
                (count_hbm, count_ref),
                (hubs_hbm, hubs_ref),
            )
        )
    ]
    for q in (0, 1, 6, 7, 8, 2, 3, 4, 5):
        loads[q].start()

    barrier = pltpu.get_barrier_semaphore()
    spot = lax.rem(me, plane)
    base = me - spot
    first_in = jnp.logical_and(spot == 0, me > 0)
    last_in = jnp.logical_and(spot == plane - 1, me < n - 1)

    def call(sem, to):
        pl.semaphore_signal(sem, inc=1, device_id=(to,), device_id_type=MESH)

    def across(sem):
        def one(step, carry):
            call(sem, lax.rem(me + step * plane, n))
            return carry

        lax.fori_loop(1, planes, one, 0)

    def greet(step, carry):
        call(barrier, base + lax.rem(spot + step, plane))
        return carry

    across(barrier)

    @pl.when(first_in)
    def _():
        call(barrier, me - 1)

    @pl.when(last_in)
    def _():
        call(barrier, me + 1)

    lax.fori_loop(1, plane, greet, 0)

    loads[0].wait()
    roots = lax.rsqrt(degree[...].astype(jnp.float32)).T
    for b in range(blocks):
        inv[b] = jnp.broadcast_to(roots[:, b : b + 1], (tile, LANES))

    def wide(b, width):
        return jnp.concatenate([inv[b]] * (width // LANES), axis=1)

    @pl.when(me == 0)
    def _():
        for i in range(pairs):
            exts[i][blocks : blocks + send_most] = jnp.zeros((send_most,) + exts[i].shape[1:], jnp.bfloat16)

    @pl.when(me == n - 1)
    def _():
        for i in range(pairs):
            exts[i][blocks + send_most :] = jnp.zeros((send_most,) + exts[i].shape[1:], jnp.bfloat16)

    def rim_copy(i, side):
        first = blocks if side == 1 else blocks + send_most
        to = me + 1 if side == 1 else me - 1
        return pltpu.make_async_remote_copy(
            src_ref=sends[i].at[side],
            dst_ref=exts[i].at[pl.ds(first, send_most)],
            send_sem=rim_send_sem.at[i, side],
            recv_sem=rim_recv_sem.at[i, side],
            device_id=(to,),
            device_id_type=MESH,
        )

    def stage(i):
        source = locals_[i]
        picked = []
        for q in range(hub_dev):
            row = hubs_ref[q]
            near = groups[i][lax.div(row, 16)].astype(jnp.float32)
            here = lax.broadcasted_iota(jnp.int32, near.shape, 0) == lax.rem(row, 16)
            picked.append(jnp.sum(jnp.where(here, near, 0.0), axis=0, keepdims=True))
        packed = jnp.concatenate(picked, axis=0).astype(jnp.bfloat16)
        hub_sends[i][...] = packed
        hub_bufs[i][me] = packed

        for side in range(2):
            for s in range(send_most):
                block = source[listed_ref[0, side, s]]
                keep = jnp.where(s < count_ref[0, side], 1.0, 0.0).astype(jnp.float32)
                sends[i][side, s] = (block.astype(jnp.float32) * keep).astype(jnp.bfloat16)


    def launch_hubs(i):
        def spread(step, carry):
            pltpu.make_async_remote_copy(
                src_ref=hub_sends[i],
                dst_ref=hub_bufs[i].at[me],
                send_sem=hub_send_sem.at[i],
                recv_sem=hub_recv_sem.at[i],
                device_id=(lax.rem(me + step, n),),
                device_id_type=MESH,
            ).start()
            return carry

        lax.fori_loop(1, n, spread, 0)

    def launch_rims(i):
        @pl.when(me < n - 1)
        def _():
            rim_copy(i, 1).start()

        @pl.when(me > 0)
        def _():
            rim_copy(i, 0).start()

    def prepare(c):
        which, at, width = pieces[c]

        def one(b, carry):
            rows = pl.ds(pl.multiple_of(b * tile, tile), tile)
            x = (features, embeddings)[which][rows, at : at + width]
            z = (x.astype(jnp.float32) * wide(b, width)).astype(jnp.bfloat16)
            locals_[c][b] = z
            groups[c][pl.ds(b * per, per)] = z.reshape(per, 16, width)
            exts[c][b] = z
            return carry

        lax.fori_loop(0, blocks, one, 0, unroll=UNROLL)

    more = first_in.astype(jnp.int32) + last_in.astype(jnp.int32)
    with jax.named_scope("group"):
        pl.semaphore_wait(barrier, planes + plane - 2 + more)
    across(ready)
    with jax.named_scope("loads"):
        for q in (6, 7, 8, 1, 2):
            loads[q].wait()
    with jax.named_scope("prepare"):
        prepare(0)
        stage(0)
        launch_rims(0)
        for c in range(1, chunks):
            prepare(c)
            stage(c)
        loads[3].wait()
        loads[4].wait()
        loads[5].wait()
        weight[...] = weight_t[...].T
    with jax.named_scope("ready"):
        pl.semaphore_wait(ready, planes - 1)
    with jax.named_scope("launch"):
        for c in range(chunks):
            launch_hubs(c)
        for c in range(1, chunks):
            launch_rims(c)

    def drain(i, sem):
        some = hub_bufs[i].at[pl.ds(0, n - 1)]
        pltpu.make_async_copy(some, some, sem.at[i]).wait()

    for hop in range(HOPS):
        for c in range(chunks):
            i = hop * chunks + c
            j = i + chunks
            which, at, width = pieces[c]
            with jax.named_scope(f"hubwait_{hop}_{c}"):
                drain(i, hub_recv_sem)
            with jax.named_scope(f"rimwait_{hop}_{c}"):

                @pl.when(me > 0)
                def _():
                    rim_copy(i, 1).wait_recv()

                @pl.when(me < n - 1)
                def _():
                    rim_copy(i, 0).wait_recv()

            hubs = hub_bufs[i][...].reshape(n * hub_dev, width)

            def one(b, carry):
                rows = pl.ds(pl.multiple_of(b * tile, tile), tile)
                left = jnp.concatenate([tiles[b, k] for k in range(taps)], axis=1)
                right = jnp.concatenate(
                    [exts[i][cols_ref[k, b]] for k in range(taps)], axis=0
                )
                y = jnp.dot(left, right, preferred_element_type=jnp.float32)
                y = y + jnp.dot(weight[rows, :], hubs, preferred_element_type=jnp.float32)
                root = wide(b, width)
                x = (y * root).astype(jnp.bfloat16)
                (out_f, out_e)[which][hop, rows, at : at + width] = x
                if hop + 1 < HOPS:
                    z = (x.astype(jnp.float32) * root).astype(jnp.bfloat16)
                    locals_[j][b] = z
                    groups[j][pl.ds(b * per, per)] = z.reshape(per, 16, width)
                    exts[j][b] = z
                return carry

            with jax.named_scope(f"compute_{hop}_{c}"):
                lax.fori_loop(0, blocks, one, 0, unroll=UNROLL)
            if hop + 1 < HOPS:
                with jax.named_scope(f"launch_{hop}_{c}"):
                    stage(j)
                    launch_hubs(j)
                    launch_rims(j)

    with jax.named_scope("drain"):
        for i in range(pairs):
            drain(i, hub_send_sem)

            @pl.when(me < n - 1)
            def _():
                rim_copy(i, 1).wait_send()

            @pl.when(me > 0)
            def _():
                rim_copy(i, 0).wait_send()


def group_of(n):
    size = 1
    while size * size < n:
        size *= 2
    return size if n % size == 0 else n


def flush(held_f, held_e, out_f, out_e, sem):
    copies = [
        pltpu.make_async_copy(held_f, out_f, sem.at[0]),
        pltpu.make_async_copy(held_e, out_e, sem.at[1]),
    ]
    for copy in copies:
        copy.start()
    for copy in copies:
        copy.wait()


def body(
    features, embeddings, tile_values, tile_columns, send_blocks, send_count,
    hub_rows, hub_weight, degree,
):
    n = lax.axis_size("dom")
    rows = features.shape[0]
    blocks, taps, tile, _ = tile_values.shape
    send_most = send_blocks.shape[2]
    hub_dev = hub_rows.shape[0]
    pieces = cut(0, features.shape[1]) + cut(1, embeddings.shape[1])
    sizes = (blocks, tile, taps, send_most, hub_dev, pieces, group_of(n))
    widths = [width for _, _, width in pieces] * HOPS
    out_bytes = HOPS * rows * (features.shape[1] + embeddings.shape[1]) * 2
    vmem = pl.BlockSpec(memory_space=pltpu.VMEM)
    bf16 = jnp.bfloat16
    held = pl.pallas_call(
        functools.partial(kernel, n, sizes),
        out_shape=(
            pltpu.VMEM((HOPS, rows, features.shape[1]), bf16),
            pltpu.VMEM((HOPS, rows, embeddings.shape[1]), bf16),
        ),
        in_specs=[pl.BlockSpec(memory_space=pltpu.HBM)] * 9,
        out_specs=(vmem, vmem),
        scratch_shapes=[
            pltpu.VMEM(shape + (width,), bf16)
            for shape in (
                (blocks, tile),
                (rows // 16, 16),
                (blocks + 2 * send_most, tile),
                (2, send_most, tile),
                (hub_dev,),
                (n, hub_dev),
            )
            for width in widths
        ]
        + [
            pltpu.SMEM((taps, blocks), jnp.int32),
            pltpu.SMEM(send_blocks.shape, jnp.int32),
            pltpu.SMEM(send_count.shape, jnp.int32),
            pltpu.SMEM(hub_rows.shape, jnp.int32),
            pltpu.VMEM(features.shape, bf16),
            pltpu.VMEM(embeddings.shape, bf16),
            pltpu.VMEM(tile_values.shape, bf16),
            pltpu.VMEM((n * hub_dev, rows), bf16),
            pltpu.VMEM((blocks, tile), jnp.int32),
            pltpu.VMEM((rows, n * hub_dev), bf16),
            pltpu.VMEM((blocks, tile, LANES), jnp.float32),
            pltpu.SemaphoreType.DMA((9,)),
            pltpu.SemaphoreType.DMA((len(widths), 2)),
            pltpu.SemaphoreType.DMA((len(widths), 2)),
            pltpu.SemaphoreType.DMA((len(widths),)),
            pltpu.SemaphoreType.DMA((len(widths),)),
            pltpu.SemaphoreType.REGULAR,
        ],
        compiler_params=pltpu.CompilerParams(
            collective_id=0, has_side_effects=True, vmem_limit_bytes=VMEM - out_bytes
        ),
    )(
        tile_columns.T, send_blocks, send_count, hub_rows,
        features, embeddings, tile_values, hub_weight.T,
        degree.reshape(blocks, tile),
    )
    hbm = pl.BlockSpec(memory_space=pltpu.HBM)
    return pl.pallas_call(
        flush,
        out_shape=tuple(jax.ShapeDtypeStruct(h.shape, h.dtype) for h in held),
        in_specs=[vmem] * 2,
        out_specs=(hbm, hbm),
        scratch_shapes=[pltpu.SemaphoreType.DMA((2,))],
        compiler_params=pltpu.CompilerParams(vmem_limit_bytes=2**20),
    )(*held)


def solution(mesh):
    placed = (
        P("dom", None),
        P("dom", None),
        P("dom", None, None, None),
        P("dom", None),
        P("dom", None, None),
        P("dom", None),
        P("dom"),
        P("dom", None),
        P("dom"),
    )
    return jax.shard_map(
        body,
        mesh=mesh,
        in_specs=placed,
        out_specs=(P(None, "dom", None), P(None, "dom", None)),
        check_vma=False,
    )
```

```python
import functools

import jax
import jax.numpy as jnp
from jax import lax
from jax.experimental import pallas as pl
from jax.experimental.pallas import tpu as pltpu
from jax.sharding import PartitionSpec as P

HOPS = 3
LANES = 128
WIDTH = 256
UNROLL = 4
VMEM = 67043328
MESH = pl.DeviceIdType.MESH


def cut(which, columns):
    return [(which, at, min(WIDTH, columns - at)) for at in range(0, columns, WIDTH)]


def kernel(
    n, sizes, cols_hbm, listed_hbm, count_hbm, hubs_hbm,
    features_hbm, embeddings_hbm, tiles_hbm, weight_hbm, degree_hbm,
    out_f, out_e, *scratch,
):
    blocks, tile, taps, send_most, hub_dev, pieces = sizes
    chunks = len(pieces)
    per = tile // 16
    pairs = HOPS * chunks
    scratch = list(scratch)
    take = lambda count: [scratch.pop(0) for _ in range(count)]
    locals_, groups, exts, sends, hub_sends, hub_bufs = (take(pairs) for _ in range(6))
    (
        cols_ref, listed_ref, count_ref, hubs_ref,
        features, embeddings, tiles, weight_t, degree, weight, inv,
        load_sem, rim_send_sem, rim_recv_sem, hub_send_sem, hub_recv_sem,
    ) = scratch
    me = lax.axis_index("dom")

    loads = [
        pltpu.make_async_copy(source, held, load_sem.at[q])
        for q, (source, held) in enumerate(
            (
                (degree_hbm, degree),
                (features_hbm, features),
                (embeddings_hbm, embeddings),
                (tiles_hbm, tiles),
                (weight_hbm, weight_t),
                (cols_hbm, cols_ref),
                (listed_hbm, listed_ref),
                (count_hbm, count_ref),
                (hubs_hbm, hubs_ref),
            )
        )
    ]
    barrier = pltpu.get_barrier_semaphore()

    def greet(step, carry):
        pl.semaphore_signal(
            barrier, inc=1, device_id=(lax.rem(me + step, n),), device_id_type=MESH
        )
        return carry

    loads[0].start()
    loads[1].start()
    lax.fori_loop(1, n, greet, 0)
    for q in (6, 7, 8, 2, 3, 4, 5):
        loads[q].start()

    loads[0].wait()
    roots = lax.rsqrt(degree[...].astype(jnp.float32)).T
    for b in range(blocks):
        inv[b] = jnp.broadcast_to(roots[:, b : b + 1], (tile, LANES))

    def wide(b, width):
        return jnp.concatenate([inv[b]] * (width // LANES), axis=1)

    @pl.when(me == 0)
    def _():
        for i in range(pairs):
            exts[i][blocks : blocks + send_most] = jnp.zeros((send_most,) + exts[i].shape[1:], jnp.bfloat16)

    @pl.when(me == n - 1)
    def _():
        for i in range(pairs):
            exts[i][blocks + send_most :] = jnp.zeros((send_most,) + exts[i].shape[1:], jnp.bfloat16)

    def rim_copy(i, side):
        first = blocks if side == 1 else blocks + send_most
        to = me + 1 if side == 1 else me - 1
        return pltpu.make_async_remote_copy(
            src_ref=sends[i].at[side],
            dst_ref=exts[i].at[pl.ds(first, send_most)],
            send_sem=rim_send_sem.at[i, side],
            recv_sem=rim_recv_sem.at[i, side],
            device_id=(to,),
            device_id_type=MESH,
        )

    def stage(i):
        source = locals_[i]
        picked = []
        for q in range(hub_dev):
            row = hubs_ref[q]
            near = groups[i][lax.div(row, 16)].astype(jnp.float32)
            here = lax.broadcasted_iota(jnp.int32, near.shape, 0) == lax.rem(row, 16)
            picked.append(jnp.sum(jnp.where(here, near, 0.0), axis=0, keepdims=True))
        packed = jnp.concatenate(picked, axis=0).astype(jnp.bfloat16)
        hub_sends[i][...] = packed
        hub_bufs[i][me] = packed

        for side in range(2):
            for s in range(send_most):
                block = source[listed_ref[0, side, s]]
                keep = jnp.where(s < count_ref[0, side], 1.0, 0.0).astype(jnp.float32)
                sends[i][side, s] = (block.astype(jnp.float32) * keep).astype(jnp.bfloat16)


    def launch_hubs(i):
        def spread(step, carry):
            pltpu.make_async_remote_copy(
                src_ref=hub_sends[i],
                dst_ref=hub_bufs[i].at[me],
                send_sem=hub_send_sem.at[i],
                recv_sem=hub_recv_sem.at[i],
                device_id=(lax.rem(me + step, n),),
                device_id_type=MESH,
            ).start()
            return carry

        lax.fori_loop(1, n, spread, 0)

    def launch_rims(i):
        @pl.when(me < n - 1)
        def _():
            rim_copy(i, 1).start()

        @pl.when(me > 0)
        def _():
            rim_copy(i, 0).start()

    def prepare(c):
        which, at, width = pieces[c]

        def one(b, carry):
            rows = pl.ds(pl.multiple_of(b * tile, tile), tile)
            x = (features, embeddings)[which][rows, at : at + width]
            z = (x.astype(jnp.float32) * wide(b, width)).astype(jnp.bfloat16)
            locals_[c][b] = z
            groups[c][pl.ds(b * per, per)] = z.reshape(per, 16, width)
            exts[c][b] = z
            return carry

        lax.fori_loop(0, blocks, one, 0, unroll=UNROLL)

    for q in (6, 7, 8, 1, 2):
        loads[q].wait()
    with jax.named_scope("prepare"):
        for c in range(chunks):
            prepare(c)
            stage(c)
    with jax.named_scope("barrier"):
        pl.semaphore_wait(barrier, n - 1)
    with jax.named_scope("launch"):
        for c in range(chunks):
            launch_hubs(c)
            launch_rims(c)

    with jax.named_scope("weights"):
        for q in (3, 4, 5):
            loads[q].wait()
        weight[...] = weight_t[...].T

    def drain(i, sem):
        some = hub_bufs[i].at[pl.ds(0, n - 1)]
        pltpu.make_async_copy(some, some, sem.at[i]).wait()

    for hop in range(HOPS):
        for c in range(chunks):
            i = hop * chunks + c
            j = i + chunks
            which, at, width = pieces[c]
            with jax.named_scope(f"hubwait_{hop}_{c}"):
                drain(i, hub_recv_sem)
            with jax.named_scope(f"rimwait_{hop}_{c}"):

                @pl.when(me > 0)
                def _():
                    rim_copy(i, 1).wait_recv()

                @pl.when(me < n - 1)
                def _():
                    rim_copy(i, 0).wait_recv()

            hubs = hub_bufs[i][...].reshape(n * hub_dev, width)

            def one(b, carry):
                rows = pl.ds(pl.multiple_of(b * tile, tile), tile)
                left = jnp.concatenate([tiles[b, k] for k in range(taps)], axis=1)
                right = jnp.concatenate(
                    [exts[i][cols_ref[k, b]] for k in range(taps)], axis=0
                )
                y = jnp.dot(left, right, preferred_element_type=jnp.float32)
                y = y + jnp.dot(weight[rows, :], hubs, preferred_element_type=jnp.float32)
                root = wide(b, width)
                x = (y * root).astype(jnp.bfloat16)
                (out_f, out_e)[which][hop, rows, at : at + width] = x
                if hop + 1 < HOPS:
                    z = (x.astype(jnp.float32) * root).astype(jnp.bfloat16)
                    locals_[j][b] = z
                    groups[j][pl.ds(b * per, per)] = z.reshape(per, 16, width)
                    exts[j][b] = z
                return carry

            with jax.named_scope(f"compute_{hop}_{c}"):
                lax.fori_loop(0, blocks, one, 0, unroll=UNROLL)
            if hop + 1 < HOPS:
                with jax.named_scope(f"launch_{hop}_{c}"):
                    stage(j)
                    launch_hubs(j)
                    launch_rims(j)

    with jax.named_scope("drain"):
        for i in range(pairs):
            drain(i, hub_send_sem)

            @pl.when(me < n - 1)
            def _():
                rim_copy(i, 1).wait_send()

            @pl.when(me > 0)
            def _():
                rim_copy(i, 0).wait_send()


def flush(held_f, held_e, out_f, out_e, sem):
    copies = [
        pltpu.make_async_copy(held_f, out_f, sem.at[0]),
        pltpu.make_async_copy(held_e, out_e, sem.at[1]),
    ]
    for copy in copies:
        copy.start()
    for copy in copies:
        copy.wait()


def body(
    features, embeddings, tile_values, tile_columns, send_blocks, send_count,
    hub_rows, hub_weight, degree,
):
    n = lax.axis_size("dom")
    rows = features.shape[0]
    blocks, taps, tile, _ = tile_values.shape
    send_most = send_blocks.shape[2]
    hub_dev = hub_rows.shape[0]
    pieces = cut(0, features.shape[1]) + cut(1, embeddings.shape[1])
    sizes = (blocks, tile, taps, send_most, hub_dev, pieces)
    widths = [width for _, _, width in pieces] * HOPS
    out_bytes = HOPS * rows * (features.shape[1] + embeddings.shape[1]) * 2
    vmem = pl.BlockSpec(memory_space=pltpu.VMEM)
    bf16 = jnp.bfloat16
    held = pl.pallas_call(
        functools.partial(kernel, n, sizes),
        out_shape=(
            pltpu.VMEM((HOPS, rows, features.shape[1]), bf16),
            pltpu.VMEM((HOPS, rows, embeddings.shape[1]), bf16),
        ),
        in_specs=[pl.BlockSpec(memory_space=pltpu.HBM)] * 9,
        out_specs=(vmem, vmem),
        scratch_shapes=[
            pltpu.VMEM(shape + (width,), bf16)
            for shape in (
                (blocks, tile),
                (rows // 16, 16),
                (blocks + 2 * send_most, tile),
                (2, send_most, tile),
                (hub_dev,),
                (n, hub_dev),
            )
            for width in widths
        ]
        + [
            pltpu.SMEM((taps, blocks), jnp.int32),
            pltpu.SMEM(send_blocks.shape, jnp.int32),
            pltpu.SMEM(send_count.shape, jnp.int32),
            pltpu.SMEM(hub_rows.shape, jnp.int32),
            pltpu.VMEM(features.shape, bf16),
            pltpu.VMEM(embeddings.shape, bf16),
            pltpu.VMEM(tile_values.shape, bf16),
            pltpu.VMEM((n * hub_dev, rows), bf16),
            pltpu.VMEM((blocks, tile), jnp.int32),
            pltpu.VMEM((rows, n * hub_dev), bf16),
            pltpu.VMEM((blocks, tile, LANES), jnp.float32),
            pltpu.SemaphoreType.DMA((9,)),
            pltpu.SemaphoreType.DMA((len(widths), 2)),
            pltpu.SemaphoreType.DMA((len(widths), 2)),
            pltpu.SemaphoreType.DMA((len(widths),)),
            pltpu.SemaphoreType.DMA((len(widths),)),
        ],
        compiler_params=pltpu.CompilerParams(
            collective_id=0, has_side_effects=True, vmem_limit_bytes=VMEM - out_bytes
        ),
    )(
        tile_columns.T, send_blocks, send_count, hub_rows,
        features, embeddings, tile_values, hub_weight.T,
        degree.reshape(blocks, tile),
    )
    hbm = pl.BlockSpec(memory_space=pltpu.HBM)
    return pl.pallas_call(
        flush,
        out_shape=tuple(jax.ShapeDtypeStruct(h.shape, h.dtype) for h in held),
        in_specs=[vmem] * 2,
        out_specs=(hbm, hbm),
        scratch_shapes=[pltpu.SemaphoreType.DMA((2,))],
        compiler_params=pltpu.CompilerParams(vmem_limit_bytes=2**20),
    )(*held)


def solution(mesh):
    placed = (
        P("dom", None),
        P("dom", None),
        P("dom", None, None, None),
        P("dom", None),
        P("dom", None, None),
        P("dom", None),
        P("dom"),
        P("dom", None),
        P("dom"),
    )
    return jax.shard_map(
        body,
        mesh=mesh,
        in_specs=placed,
        out_specs=(P(None, "dom", None), P(None, "dom", None)),
        check_vma=False,
    )
```

```python
import functools

import jax
import jax.numpy as jnp
from jax import lax
from jax.experimental import pallas as pl
from jax.experimental.pallas import tpu as pltpu
from jax.sharding import PartitionSpec as P

HOPS = 3
LANES = 128
WIDTH = 256
UNROLL = 4
VMEM = 67043328
MESH = pl.DeviceIdType.MESH


def cut(which, columns):
    return [(which, at, min(WIDTH, columns - at)) for at in range(0, columns, WIDTH)]


def kernel(
    n, sizes, cols_hbm, listed_hbm, count_hbm, hubs_hbm,
    features_hbm, embeddings_hbm, tiles_hbm, weight_hbm, degree_hbm,
    out_f, out_e, *scratch,
):
    blocks, tile, taps, send_most, hub_dev, pieces = sizes
    chunks = len(pieces)
    per = tile // 16
    pairs = HOPS * chunks
    scratch = list(scratch)
    take = lambda count: [scratch.pop(0) for _ in range(count)]
    locals_, groups, exts, sends, hub_sends, hub_bufs = (take(pairs) for _ in range(6))
    (
        cols_ref, listed_ref, count_ref, hubs_ref,
        features, embeddings, tiles, weight_t, degree, weight, inv,
        load_sem, rim_send_sem, rim_recv_sem, hub_send_sem, hub_recv_sem,
    ) = scratch
    me = lax.axis_index("dom")

    def load(source, held, q):
        return pltpu.make_async_copy(source, held, load_sem.at[q])

    load_degree = load(degree_hbm, degree, 0)
    load_features = load(features_hbm, features, 1)
    load_embeddings = load(embeddings_hbm, embeddings, 2)
    small = [
        load(listed_hbm, listed_ref, 3),
        load(count_hbm, count_ref, 4),
        load(hubs_hbm, hubs_ref, 5),
    ]
    late = [
        load(tiles_hbm, tiles, 0),
        load(weight_hbm, weight_t, 1),
        load(cols_hbm, cols_ref, 2),
    ]
    for copy in [load_degree, load_features, load_embeddings] + small:
        copy.start()

    barrier = pltpu.get_barrier_semaphore()

    def greet(step, carry):
        to = lax.rem(me + step, n)
        pl.semaphore_signal(barrier, inc=1, device_id=(to,), device_id_type=MESH)
        return carry

    lax.fori_loop(1, n, greet, 0)

    @pl.when(me == 0)
    def _():
        for i in range(pairs):
            exts[i][blocks : blocks + send_most] = jnp.zeros((send_most,) + exts[i].shape[1:], jnp.bfloat16)

    @pl.when(me == n - 1)
    def _():
        for i in range(pairs):
            exts[i][blocks + send_most :] = jnp.zeros((send_most,) + exts[i].shape[1:], jnp.bfloat16)

    load_degree.wait()
    roots = lax.rsqrt(degree[...].astype(jnp.float32)).T
    for b in range(blocks):
        inv[b] = jnp.broadcast_to(roots[:, b : b + 1], (tile, LANES))

    def wide(root, width):
        return jnp.concatenate([root] * (width // LANES), axis=1)

    def rim_copy(i, side):
        first = blocks if side == 1 else blocks + send_most
        to = me + 1 if side == 1 else me - 1
        return pltpu.make_async_remote_copy(
            src_ref=sends[i].at[side],
            dst_ref=exts[i].at[pl.ds(first, send_most)],
            send_sem=rim_send_sem.at[i % chunks],
            recv_sem=rim_recv_sem.at[i % (2 * chunks)],
            device_id=(to,),
            device_id_type=MESH,
        )

    inner = jnp.logical_and(me > 0, me < n - 1)

    def rim_wait(i, sem):
        def of(count):
            some = exts[i].at[pl.ds(blocks, count)]
            return pltpu.make_async_copy(some, some, sem)

        @pl.when(inner)
        def _():
            of(2 * send_most).wait()

        @pl.when(jnp.logical_not(inner))
        def _():
            of(send_most).wait()

    def hub_wait(i, sem):
        some = hub_bufs[i].at[pl.ds(0, n - 1)]
        pltpu.make_async_copy(some, some, sem).wait()

    def row_of(rows, row):
        here = lax.broadcasted_iota(jnp.int32, rows.shape, 0) == lax.rem(row, 16)
        return jnp.sum(jnp.where(here, rows.astype(jnp.float32), 0.0), axis=0, keepdims=True)

    def stage_rims(i):
        for side in range(2):
            for s in range(send_most):
                block = locals_[i][listed_ref[0, side, s]]
                keep = jnp.where(s < count_ref[0, side], 1.0, 0.0).astype(jnp.float32)
                sends[i][side, s] = (block.astype(jnp.float32) * keep).astype(jnp.bfloat16)

    def stage_hubs(i):
        near = [groups[i][lax.div(hubs_ref[q], 16)] for q in range(hub_dev)]
        picked = [row_of(near[q], hubs_ref[q]) for q in range(hub_dev)]
        packed = jnp.concatenate(picked, axis=0).astype(jnp.bfloat16)
        hub_sends[i][...] = packed
        hub_bufs[i][me] = packed

    def launch_rims(i):
        @pl.when(me < n - 1)
        def _():
            rim_copy(i, 1).start()

        @pl.when(me > 0)
        def _():
            rim_copy(i, 0).start()

    def launch_hubs(i):
        def spread(step, carry):
            pltpu.make_async_remote_copy(
                src_ref=hub_sends[i],
                dst_ref=hub_bufs[i].at[me],
                send_sem=hub_send_sem.at[i % chunks],
                recv_sem=hub_recv_sem.at[i % (2 * chunks)],
                device_id=(lax.rem(me + step, n),),
                device_id_type=MESH,
            ).start()
            return carry

        lax.fori_loop(1, n, spread, 0)

    def prepare(c):
        which, at, width = pieces[c]

        def one(b, carry):
            rows = pl.ds(pl.multiple_of(b * tile, tile), tile)
            x = (features, embeddings)[which][rows, at : at + width]
            z = (x.astype(jnp.float32) * wide(inv[b], width)).astype(jnp.bfloat16)
            locals_[c][b] = z
            groups[c][pl.ds(b * per, per)] = z.reshape(per, 16, width)
            exts[c][b] = z
            return carry

        lax.fori_loop(0, blocks, one, 0, unroll=UNROLL)

    for copy in small + [load_features, load_embeddings]:
        copy.wait()
    for copy in late:
        copy.start()

    for c in range(chunks):
        with jax.named_scope("prepare"):
            prepare(c)
            stage_hubs(c)
            stage_rims(c)
        if c == 0:
            with jax.named_scope("barrier"):
                pl.semaphore_wait(barrier, n - 1)
        with jax.named_scope("launch"):
            launch_hubs(c)
            launch_rims(c)
    with jax.named_scope("weights"):
        for copy in late:
            copy.wait()
        weight[...] = weight_t[...].T

    for hop in range(HOPS):
        for c in range(chunks):
            i = hop * chunks + c
            j = i + chunks
            which, at, width = pieces[c]
            with jax.named_scope(f"hubwait_{hop}_{c}"):
                hub_wait(i, hub_recv_sem.at[i % (2 * chunks)])
            with jax.named_scope(f"rimwait_{hop}_{c}"):
                rim_wait(i, rim_recv_sem.at[i % (2 * chunks)])

            hubs = hub_bufs[i][...].reshape(n * hub_dev, width)

            def one(b, carry):
                rows = pl.ds(pl.multiple_of(b * tile, tile), tile)
                left = jnp.concatenate([tiles[b, k] for k in range(taps)], axis=1)
                right = jnp.concatenate(
                    [exts[i][cols_ref[k, b]] for k in range(taps)], axis=0
                )
                y = jnp.dot(left, right, preferred_element_type=jnp.float32)
                y = y + jnp.dot(weight[rows, :], hubs, preferred_element_type=jnp.float32)
                root = wide(inv[b], width)
                x = (y * root).astype(jnp.bfloat16)
                (out_f, out_e)[which][hop, rows, at : at + width] = x
                if hop + 1 < HOPS:
                    z = (x.astype(jnp.float32) * root).astype(jnp.bfloat16)
                    locals_[j][b] = z
                    groups[j][pl.ds(b * per, per)] = z.reshape(per, 16, width)
                    exts[j][b] = z
                return carry

            with jax.named_scope(f"compute_{hop}_{c}"):
                lax.fori_loop(0, blocks, one, 0, unroll=UNROLL)
            if hop + 1 < HOPS:
                with jax.named_scope(f"launch_{hop}_{c}"):
                    stage_hubs(j)
                    hub_wait(i, hub_send_sem.at[c])
                    launch_hubs(j)
                    stage_rims(j)
                    rim_wait(i, rim_send_sem.at[c])
                    launch_rims(j)

    with jax.named_scope("drain"):
        for i in range(pairs - chunks, pairs):
            hub_wait(i, hub_send_sem.at[i % chunks])
            rim_wait(i, rim_send_sem.at[i % chunks])


def flush(held_f, held_e, out_f, out_e, sem):
    copies = [
        pltpu.make_async_copy(held_f, out_f, sem.at[0]),
        pltpu.make_async_copy(held_e, out_e, sem.at[1]),
    ]
    for copy in copies:
        copy.start()
    for copy in copies:
        copy.wait()


def body(
    features, embeddings, tile_values, tile_columns, send_blocks, send_count,
    hub_rows, hub_weight, degree,
):
    n = lax.axis_size("dom")
    rows = features.shape[0]
    blocks, taps, tile, _ = tile_values.shape
    send_most = send_blocks.shape[2]
    hub_dev = hub_rows.shape[0]
    pieces = cut(0, features.shape[1]) + cut(1, embeddings.shape[1])
    columns = features.shape[1] + embeddings.shape[1]
    sizes = (blocks, tile, taps, send_most, hub_dev, pieces)
    widths = [width for _, _, width in pieces] * HOPS
    out_bytes = HOPS * rows * columns * 2
    vmem = pl.BlockSpec(memory_space=pltpu.VMEM)
    bf16 = jnp.bfloat16
    held = pl.pallas_call(
        functools.partial(kernel, n, sizes),
        out_shape=(
            pltpu.VMEM((HOPS, rows, features.shape[1]), bf16),
            pltpu.VMEM((HOPS, rows, embeddings.shape[1]), bf16),
        ),
        in_specs=[pl.BlockSpec(memory_space=pltpu.HBM)] * 9,
        out_specs=(vmem, vmem),
        scratch_shapes=[
            pltpu.VMEM(shape + (width,), bf16)
            for shape in (
                (blocks, tile),
                (rows // 16, 16),
                (blocks + 2 * send_most, tile),
                (2, send_most, tile),
                (hub_dev,),
                (n, hub_dev),
            )
            for width in widths
        ]
        + [
            pltpu.SMEM((taps, blocks), jnp.int32),
            pltpu.SMEM(send_blocks.shape, jnp.int32),
            pltpu.SMEM(send_count.shape, jnp.int32),
            pltpu.SMEM(hub_rows.shape, jnp.int32),
            pltpu.VMEM(features.shape, bf16),
            pltpu.VMEM(embeddings.shape, bf16),
            pltpu.VMEM(tile_values.shape, bf16),
            pltpu.VMEM((n * hub_dev, rows), bf16),
            pltpu.VMEM((blocks, tile), jnp.int32),
            pltpu.VMEM((rows, n * hub_dev), bf16),
            pltpu.VMEM((blocks, tile, LANES), jnp.float32),
            pltpu.SemaphoreType.DMA((6,)),
            pltpu.SemaphoreType.DMA((len(pieces),)),
            pltpu.SemaphoreType.DMA((2 * len(pieces),)),
            pltpu.SemaphoreType.DMA((len(pieces),)),
            pltpu.SemaphoreType.DMA((2 * len(pieces),)),
        ],
        compiler_params=pltpu.CompilerParams(
            collective_id=0, has_side_effects=True, vmem_limit_bytes=VMEM - out_bytes
        ),
    )(
        tile_columns.T, send_blocks, send_count, hub_rows,
        features, embeddings, tile_values, hub_weight.T,
        degree.reshape(blocks, tile),
    )
    hbm = pl.BlockSpec(memory_space=pltpu.HBM)
    return pl.pallas_call(
        flush,
        out_shape=tuple(jax.ShapeDtypeStruct(h.shape, h.dtype) for h in held),
        in_specs=[vmem] * 2,
        out_specs=(hbm, hbm),
        scratch_shapes=[pltpu.SemaphoreType.DMA((2,))],
        compiler_params=pltpu.CompilerParams(vmem_limit_bytes=2**20),
    )(*held)


def solution(mesh):
    placed = (
        P("dom", None),
        P("dom", None),
        P("dom", None, None, None),
        P("dom", None),
        P("dom", None, None),
        P("dom", None),
        P("dom"),
        P("dom", None),
        P("dom"),
    )
    return jax.shard_map(
        body,
        mesh=mesh,
        in_specs=placed,
        out_specs=(P(None, "dom", None), P(None, "dom", None)),
        check_vma=False,
    )
```

```python
import functools

import jax
import jax.numpy as jnp
from jax import lax
from jax.experimental import pallas as pl
from jax.experimental.pallas import tpu as pltpu
from jax.sharding import PartitionSpec as P

HOPS = 3
LANES = 128
WIDTH = 256
UNROLL = 4
VMEM = 67043328
MESH = pl.DeviceIdType.MESH


def cut(which, columns):
    return [(which, at, min(WIDTH, columns - at)) for at in range(0, columns, WIDTH)]


def kernel(
    n, sizes, cols_hbm, listed_hbm, count_hbm, hubs_hbm,
    features_hbm, embeddings_hbm, tiles_hbm, weight_hbm, degree_hbm,
    out_f, out_e, *scratch,
):
    blocks, tile, taps, send_most, hub_dev, pieces = sizes
    chunks = len(pieces)
    per = tile // 16
    pairs = HOPS * chunks
    scratch = list(scratch)
    take = lambda count: [scratch.pop(0) for _ in range(count)]
    locals_, groups, exts, sends, hub_sends, hub_bufs = (take(pairs) for _ in range(6))
    (
        cols_ref, listed_ref, count_ref, hubs_ref,
        features, embeddings, tiles, weight_t, degree, weight, inv,
        load_sem, rim_send_sem, rim_recv_sem, hub_send_sem, hub_recv_sem, pass_sem,
    ) = scratch
    me = lax.axis_index("dom")

    def load(source, held, q):
        return pltpu.make_async_copy(source, held, load_sem.at[q])

    load_degree = load(degree_hbm, degree, 0)
    load_features = load(features_hbm, features, 1)
    load_embeddings = load(embeddings_hbm, embeddings, 2)
    small = [
        load(listed_hbm, listed_ref, 3),
        load(count_hbm, count_ref, 4),
        load(hubs_hbm, hubs_ref, 5),
    ]
    late = [
        load(tiles_hbm, tiles, 0),
        load(weight_hbm, weight_t, 1),
        load(cols_hbm, cols_ref, 2),
    ]
    for copy in [load_degree, load_features, load_embeddings] + small:
        copy.start()

    barrier = pltpu.get_barrier_semaphore()

    quarter = n // 4
    head = me < 2 * quarter
    third = jnp.logical_and(me >= 2 * quarter, me < 3 * quarter)
    tail = me >= 3 * quarter

    def greet(step, carry):
        to = lax.rem(me + step, n)

        @pl.when(jnp.logical_not(jnp.logical_and(tail, to < 2 * quarter)))
        def _():
            pl.semaphore_signal(barrier, inc=1, device_id=(to,), device_id_type=MESH)

        return carry

    lax.fori_loop(1, n, greet, 0)

    @pl.when(me == 0)
    def _():
        for i in range(pairs):
            exts[i][blocks : blocks + send_most] = jnp.zeros((send_most,) + exts[i].shape[1:], jnp.bfloat16)

    @pl.when(me == n - 1)
    def _():
        for i in range(pairs):
            exts[i][blocks + send_most :] = jnp.zeros((send_most,) + exts[i].shape[1:], jnp.bfloat16)

    load_degree.wait()
    roots = lax.rsqrt(degree[...].astype(jnp.float32)).T
    for b in range(blocks):
        inv[b] = jnp.broadcast_to(roots[:, b : b + 1], (tile, LANES))

    def wide(root, width):
        return jnp.concatenate([root] * (width // LANES), axis=1)

    def rim_copy(i, side):
        first = blocks if side == 1 else blocks + send_most
        to = me + 1 if side == 1 else me - 1
        return pltpu.make_async_remote_copy(
            src_ref=sends[i].at[side],
            dst_ref=exts[i].at[pl.ds(first, send_most)],
            send_sem=rim_send_sem.at[i % chunks],
            recv_sem=rim_recv_sem.at[i % (2 * chunks)],
            device_id=(to,),
            device_id_type=MESH,
        )

    inner = jnp.logical_and(me > 0, me < n - 1)

    def rim_wait(i, sem):
        def of(count):
            some = exts[i].at[pl.ds(blocks, count)]
            return pltpu.make_async_copy(some, some, sem)

        @pl.when(inner)
        def _():
            of(2 * send_most).wait()

        @pl.when(jnp.logical_not(inner))
        def _():
            of(send_most).wait()

    def hub_wait(i, sem, count=n - 1):
        some = hub_bufs[i].at[pl.ds(0, count)]
        pltpu.make_async_copy(some, some, sem).wait()

    def hub_copy(i, held, owner, to, recv_sem):
        return pltpu.make_async_remote_copy(
            src_ref=held,
            dst_ref=hub_bufs[i].at[owner],
            send_sem=hub_send_sem.at[i % chunks],
            recv_sem=recv_sem,
            device_id=(to,),
            device_id_type=MESH,
        )

    def row_of(rows, row):
        here = lax.broadcasted_iota(jnp.int32, rows.shape, 0) == lax.rem(row, 16)
        return jnp.sum(jnp.where(here, rows.astype(jnp.float32), 0.0), axis=0, keepdims=True)

    def stage_rims(i):
        for side in range(2):
            for s in range(send_most):
                block = locals_[i][listed_ref[0, side, s]]
                keep = jnp.where(s < count_ref[0, side], 1.0, 0.0).astype(jnp.float32)
                sends[i][side, s] = (block.astype(jnp.float32) * keep).astype(jnp.bfloat16)

    def stage_hubs(i):
        near = [groups[i][lax.div(hubs_ref[q], 16)] for q in range(hub_dev)]
        picked = [row_of(near[q], hubs_ref[q]) for q in range(hub_dev)]
        packed = jnp.concatenate(picked, axis=0).astype(jnp.bfloat16)
        hub_sends[i][...] = packed
        hub_bufs[i][me] = packed

    def launch_rims(i):
        @pl.when(me < n - 1)
        def _():
            rim_copy(i, 1).start()

        @pl.when(me > 0)
        def _():
            rim_copy(i, 0).start()

    def launch_hubs(i):
        recv_sem = hub_recv_sem.at[i % (2 * chunks)]

        def spread(step, carry):
            hub_copy(i, hub_sends[i], me, lax.rem(me + step, n), recv_sem).start()
            return carry

        lax.fori_loop(1, n, spread, 0)

    def launch_first(c):
        recv_sem = hub_recv_sem.at[c]

        def spread(step, carry):
            hub_copy(c, hub_sends[c], me, lax.rem(me + step, n), recv_sem).start()
            return carry

        @pl.when(head)
        def _():
            source = lax.div(me, quarter)
            passer = me + (2 - source) * quarter
            hub_copy(c, hub_sends[c], me, passer, pass_sem.at[c, source]).start()

            def near(step, carry):
                to = lax.rem(me + step, 3 * quarter)

                @pl.when(to != passer)
                def _():
                    hub_copy(c, hub_sends[c], me, to, recv_sem).start()

                return carry

            lax.fori_loop(1, 3 * quarter, near, 0)

        @pl.when(jnp.logical_not(head))
        def _():
            lax.fori_loop(1, n, spread, 0)

    def pass_on(c, source):
        owner = me - (2 - source) * quarter
        hub_wait(c, pass_sem.at[c, source], 1)

        def spread(step, carry):
            to = 3 * quarter + lax.rem(me + step, quarter)
            hub_copy(c, hub_bufs[c].at[owner], owner, to, hub_recv_sem.at[c]).start()
            return carry

        lax.fori_loop(0, quarter, spread, 0)

    def first_wait(c, sem, of_head, of_third):
        @pl.when(head)
        def _():
            hub_wait(c, sem, of_head)

        @pl.when(third)
        def _():
            hub_wait(c, sem, of_third)

        @pl.when(tail)
        def _():
            hub_wait(c, sem)

    def prepare(c):
        which, at, width = pieces[c]

        def one(b, carry):
            rows = pl.ds(pl.multiple_of(b * tile, tile), tile)
            x = (features, embeddings)[which][rows, at : at + width]
            z = (x.astype(jnp.float32) * wide(inv[b], width)).astype(jnp.bfloat16)
            locals_[c][b] = z
            groups[c][pl.ds(b * per, per)] = z.reshape(per, 16, width)
            exts[c][b] = z
            return carry

        lax.fori_loop(0, blocks, one, 0, unroll=UNROLL)

    for copy in small + [load_features, load_embeddings]:
        copy.wait()
    for copy in late:
        copy.start()

    for c in range(chunks):
        with jax.named_scope("prepare"):
            prepare(c)
            stage_hubs(c)
            stage_rims(c)
        if c == 0:
            with jax.named_scope("barrier"):
                pl.semaphore_wait(barrier, n - 1 - jnp.where(head, quarter, 0))
        with jax.named_scope("launch"):
            launch_first(c)
            launch_rims(c)
    with jax.named_scope("weights"):
        for copy in late:
            copy.wait()
        weight[...] = weight_t[...].T

    @pl.when(third)
    def _():
        with jax.named_scope("pass"):
            for c in range(chunks):
                pass_on(c, 1)
                pass_on(c, 0)

    for hop in range(HOPS):
        for c in range(chunks):
            i = hop * chunks + c
            j = i + chunks
            which, at, width = pieces[c]
            with jax.named_scope(f"hubwait_{hop}_{c}"):
                if hop:
                    hub_wait(i, hub_recv_sem.at[i % (2 * chunks)])
                else:
                    first_wait(c, hub_recv_sem.at[c], n - 1, n - 3)
            with jax.named_scope(f"rimwait_{hop}_{c}"):
                rim_wait(i, rim_recv_sem.at[i % (2 * chunks)])

            hubs = hub_bufs[i][:n].reshape(n * hub_dev, width)

            def one(b, carry):
                rows = pl.ds(pl.multiple_of(b * tile, tile), tile)
                left = jnp.concatenate([tiles[b, k] for k in range(taps)], axis=1)
                right = jnp.concatenate(
                    [exts[i][cols_ref[k, b]] for k in range(taps)], axis=0
                )
                y = jnp.dot(left, right, preferred_element_type=jnp.float32)
                y = y + jnp.dot(weight[rows, :], hubs, preferred_element_type=jnp.float32)
                root = wide(inv[b], width)
                x = (y * root).astype(jnp.bfloat16)
                (out_f, out_e)[which][hop, rows, at : at + width] = x
                if hop + 1 < HOPS:
                    z = (x.astype(jnp.float32) * root).astype(jnp.bfloat16)
                    locals_[j][b] = z
                    groups[j][pl.ds(b * per, per)] = z.reshape(per, 16, width)
                    exts[j][b] = z
                return carry

            with jax.named_scope(f"compute_{hop}_{c}"):
                lax.fori_loop(0, blocks, one, 0, unroll=UNROLL)
            if hop + 1 < HOPS:
                with jax.named_scope(f"launch_{hop}_{c}"):
                    stage_hubs(j)
                    if hop:
                        hub_wait(i, hub_send_sem.at[c])
                    else:
                        first_wait(c, hub_send_sem.at[c], n - 1 - quarter, n - 1 + 2 * quarter)
                    launch_hubs(j)
                    stage_rims(j)
                    rim_wait(i, rim_send_sem.at[c])
                    launch_rims(j)

    with jax.named_scope("drain"):
        for i in range(pairs - chunks, pairs):
            hub_wait(i, hub_send_sem.at[i % chunks])
            rim_wait(i, rim_send_sem.at[i % chunks])


def flush(held_f, held_e, out_f, out_e, sem):
    copies = [
        pltpu.make_async_copy(held_f, out_f, sem.at[0]),
        pltpu.make_async_copy(held_e, out_e, sem.at[1]),
    ]
    for copy in copies:
        copy.start()
    for copy in copies:
        copy.wait()


def body(
    features, embeddings, tile_values, tile_columns, send_blocks, send_count,
    hub_rows, hub_weight, degree,
):
    n = lax.axis_size("dom")
    rows = features.shape[0]
    blocks, taps, tile, _ = tile_values.shape
    send_most = send_blocks.shape[2]
    hub_dev = hub_rows.shape[0]
    pieces = cut(0, features.shape[1]) + cut(1, embeddings.shape[1])
    columns = features.shape[1] + embeddings.shape[1]
    sizes = (blocks, tile, taps, send_most, hub_dev, pieces)
    widths = [width for _, _, width in pieces] * HOPS
    out_bytes = HOPS * rows * columns * 2
    vmem = pl.BlockSpec(memory_space=pltpu.VMEM)
    bf16 = jnp.bfloat16
    held = pl.pallas_call(
        functools.partial(kernel, n, sizes),
        out_shape=(
            pltpu.VMEM((HOPS, rows, features.shape[1]), bf16),
            pltpu.VMEM((HOPS, rows, embeddings.shape[1]), bf16),
        ),
        in_specs=[pl.BlockSpec(memory_space=pltpu.HBM)] * 9,
        out_specs=(vmem, vmem),
        scratch_shapes=[
            pltpu.VMEM(shape + (width,), bf16)
            for shape in (
                (blocks, tile),
                (rows // 16, 16),
                (blocks + 2 * send_most, tile),
                (2, send_most, tile),
                (hub_dev,),
                (n + n // 2, hub_dev),
            )
            for width in widths
        ]
        + [
            pltpu.SMEM((taps, blocks), jnp.int32),
            pltpu.SMEM(send_blocks.shape, jnp.int32),
            pltpu.SMEM(send_count.shape, jnp.int32),
            pltpu.SMEM(hub_rows.shape, jnp.int32),
            pltpu.VMEM(features.shape, bf16),
            pltpu.VMEM(embeddings.shape, bf16),
            pltpu.VMEM(tile_values.shape, bf16),
            pltpu.VMEM((n * hub_dev, rows), bf16),
            pltpu.VMEM((blocks, tile), jnp.int32),
            pltpu.VMEM((rows, n * hub_dev), bf16),
            pltpu.VMEM((blocks, tile, LANES), jnp.float32),
            pltpu.SemaphoreType.DMA((6,)),
            pltpu.SemaphoreType.DMA((len(pieces),)),
            pltpu.SemaphoreType.DMA((2 * len(pieces),)),
            pltpu.SemaphoreType.DMA((len(pieces),)),
            pltpu.SemaphoreType.DMA((2 * len(pieces),)),
            pltpu.SemaphoreType.DMA((len(pieces), 2)),
        ],
        compiler_params=pltpu.CompilerParams(
            collective_id=0, has_side_effects=True, vmem_limit_bytes=VMEM - out_bytes
        ),
    )(
        tile_columns.T, send_blocks, send_count, hub_rows,
        features, embeddings, tile_values, hub_weight.T,
        degree.reshape(blocks, tile),
    )
    hbm = pl.BlockSpec(memory_space=pltpu.HBM)
    return pl.pallas_call(
        flush,
        out_shape=tuple(jax.ShapeDtypeStruct(h.shape, h.dtype) for h in held),
        in_specs=[vmem] * 2,
        out_specs=(hbm, hbm),
        scratch_shapes=[pltpu.SemaphoreType.DMA((2,))],
        compiler_params=pltpu.CompilerParams(vmem_limit_bytes=2**20),
    )(*held)


def solution(mesh):
    placed = (
        P("dom", None),
        P("dom", None),
        P("dom", None, None, None),
        P("dom", None),
        P("dom", None, None),
        P("dom", None),
        P("dom"),
        P("dom", None),
        P("dom"),
    )
    return jax.shard_map(
        body,
        mesh=mesh,
        in_specs=placed,
        out_specs=(P(None, "dom", None), P(None, "dom", None)),
        check_vma=False,
    )
```

```python
import functools
import math

import jax
import jax.numpy as jnp
from jax import lax
from jax.experimental import pallas as pl
from jax.experimental.pallas import tpu as pltpu
from jax.sharding import PartitionSpec as P

HOPS = 3
LANES = 128
WIDTH = 256
UNROLL = 4
VMEM = 67043328
MESH = pl.DeviceIdType.MESH


def cut(which, columns):
    return [(which, at, min(WIDTH, columns - at)) for at in range(0, columns, WIDTH)]


def wide(root, width):
    return jnp.concatenate([root] * (width // LANES), axis=1)


def gathered(b, rows, taps, tiles, weight, cols, ext, hubs):
    left = jnp.concatenate([tiles[b, k] for k in range(taps)], axis=1)
    right = jnp.concatenate([ext[cols[k, b]] for k in range(taps)], axis=0)
    y = jnp.dot(left, right, preferred_element_type=jnp.float32)
    return y + jnp.dot(weight[rows, :], hubs, preferred_element_type=jnp.float32)


def kernel(
    n, sizes, cols_hbm, listed_hbm, count_hbm, hubs_hbm,
    features_hbm, embeddings_hbm, tiles_hbm, weight_hbm, degree_hbm,
    out_f, out_e, tiles, weight, inv, last_ext, last_hubs, *scratch,
):
    blocks, tile, taps, send_most, hub_dev, pieces = sizes
    chunks = len(pieces)
    per = tile // 16
    pairs = HOPS * chunks
    scratch = list(scratch)
    take = lambda count: [scratch.pop(0) for _ in range(count)]
    locals_, groups, sends, hub_sends = (take(pairs) for _ in range(4))
    exts = take(pairs - 1) + [last_ext]
    hub_bufs = take(pairs - 1) + [last_hubs]
    (
        cols_ref, listed_ref, count_ref, hubs_ref,
        features, embeddings, weight_t, degree,
        load_sem, rim_send_sem, rim_recv_sem, hub_send_sem, hub_recv_sem, pass_sem,
    ) = scratch
    me = lax.axis_index("dom")

    def load(source, held, q):
        return pltpu.make_async_copy(source, held, load_sem.at[q])

    load_degree = load(degree_hbm, degree, 0)
    load_features = load(features_hbm, features, 1)
    load_embeddings = load(embeddings_hbm, embeddings, 2)
    small = [
        load(listed_hbm, listed_ref, 3),
        load(count_hbm, count_ref, 4),
        load(hubs_hbm, hubs_ref, 5),
    ]
    late = [
        load(tiles_hbm, tiles, 0),
        load(weight_hbm, weight_t, 1),
        load(cols_hbm, cols_ref, 2),
    ]
    for copy in [load_degree, load_features, load_embeddings] + small:
        copy.start()

    barrier = pltpu.get_barrier_semaphore()

    quarter = n // 4
    head = me < 2 * quarter
    third = jnp.logical_and(me >= 2 * quarter, me < 3 * quarter)
    tail = me >= 3 * quarter

    def greet(step, carry):
        to = lax.rem(me + step, n)

        @pl.when(jnp.logical_not(jnp.logical_and(tail, to < 2 * quarter)))
        def _():
            pl.semaphore_signal(barrier, inc=1, device_id=(to,), device_id_type=MESH)

        return carry

    lax.fori_loop(1, n, greet, 0)

    @pl.when(me == 0)
    def _():
        for i in range(pairs):
            exts[i][blocks : blocks + send_most] = jnp.zeros((send_most,) + exts[i].shape[1:], jnp.bfloat16)

    @pl.when(me == n - 1)
    def _():
        for i in range(pairs):
            exts[i][blocks + send_most :] = jnp.zeros((send_most,) + exts[i].shape[1:], jnp.bfloat16)

    load_degree.wait()
    roots = lax.rsqrt(degree[...].astype(jnp.float32)).T
    for b in range(blocks):
        inv[b] = jnp.broadcast_to(roots[:, b : b + 1], (tile, LANES))

    def rim_copy(i, side):
        first = blocks if side == 1 else blocks + send_most
        to = me + 1 if side == 1 else me - 1
        return pltpu.make_async_remote_copy(
            src_ref=sends[i].at[side],
            dst_ref=exts[i].at[pl.ds(first, send_most)],
            send_sem=rim_send_sem.at[i % chunks],
            recv_sem=rim_recv_sem.at[i % (2 * chunks)],
            device_id=(to,),
            device_id_type=MESH,
        )

    inner = jnp.logical_and(me > 0, me < n - 1)

    def rim_wait(i, sem):
        def of(count):
            some = exts[i].at[pl.ds(blocks, count)]
            return pltpu.make_async_copy(some, some, sem)

        @pl.when(inner)
        def _():
            of(2 * send_most).wait()

        @pl.when(jnp.logical_not(inner))
        def _():
            of(send_most).wait()

    def hub_wait(i, sem, count=n - 1):
        some = hub_bufs[i].at[pl.ds(0, count)]
        pltpu.make_async_copy(some, some, sem).wait()

    def hub_copy(i, held, owner, to, recv_sem):
        return pltpu.make_async_remote_copy(
            src_ref=held,
            dst_ref=hub_bufs[i].at[owner],
            send_sem=hub_send_sem.at[i % chunks],
            recv_sem=recv_sem,
            device_id=(to,),
            device_id_type=MESH,
        )

    def row_of(rows, row):
        here = lax.broadcasted_iota(jnp.int32, rows.shape, 0) == lax.rem(row, 16)
        return jnp.sum(jnp.where(here, rows.astype(jnp.float32), 0.0), axis=0, keepdims=True)

    def stage_rims(i):
        for side in range(2):
            for s in range(send_most):
                block = locals_[i][listed_ref[0, side, s]]
                keep = jnp.where(s < count_ref[0, side], 1.0, 0.0).astype(jnp.float32)
                sends[i][side, s] = (block.astype(jnp.float32) * keep).astype(jnp.bfloat16)

    def stage_hubs(i):
        near = [groups[i][lax.div(hubs_ref[q], 16)] for q in range(hub_dev)]
        picked = [row_of(near[q], hubs_ref[q]) for q in range(hub_dev)]
        packed = jnp.concatenate(picked, axis=0).astype(jnp.bfloat16)
        hub_sends[i][...] = packed
        hub_bufs[i][me] = packed

    def launch_rims(i):
        @pl.when(me < n - 1)
        def _():
            rim_copy(i, 1).start()

        @pl.when(me > 0)
        def _():
            rim_copy(i, 0).start()

    def launch_hubs(i):
        recv_sem = hub_recv_sem.at[i % (2 * chunks)]

        def spread(step, carry):
            hub_copy(i, hub_sends[i], me, lax.rem(me + step, n), recv_sem).start()
            return carry

        lax.fori_loop(1, n, spread, 0)

    def launch_first(c):
        recv_sem = hub_recv_sem.at[c]

        def spread(step, carry):
            hub_copy(c, hub_sends[c], me, lax.rem(me + step, n), recv_sem).start()
            return carry

        @pl.when(head)
        def _():
            source = lax.div(me, quarter)
            passer = me + (2 - source) * quarter
            hub_copy(c, hub_sends[c], me, passer, pass_sem.at[c, source]).start()

            def near(step, carry):
                to = lax.rem(me + step, 3 * quarter)

                @pl.when(to != passer)
                def _():
                    hub_copy(c, hub_sends[c], me, to, recv_sem).start()

                return carry

            lax.fori_loop(1, 3 * quarter, near, 0)

        @pl.when(jnp.logical_not(head))
        def _():
            lax.fori_loop(1, n, spread, 0)

    def pass_on(c, source):
        owner = me - (2 - source) * quarter
        hub_wait(c, pass_sem.at[c, source], 1)

        def spread(step, carry):
            to = 3 * quarter + lax.rem(me + step, quarter)
            hub_copy(c, hub_bufs[c].at[owner], owner, to, hub_recv_sem.at[c]).start()
            return carry

        lax.fori_loop(0, quarter, spread, 0)

    def first_wait(c, sem, of_head, of_third):
        @pl.when(head)
        def _():
            hub_wait(c, sem, of_head)

        @pl.when(third)
        def _():
            hub_wait(c, sem, of_third)

        @pl.when(tail)
        def _():
            hub_wait(c, sem)

    def prepare(c):
        which, at, width = pieces[c]

        def one(b, carry):
            rows = pl.ds(pl.multiple_of(b * tile, tile), tile)
            x = (features, embeddings)[which][rows, at : at + width]
            z = (x.astype(jnp.float32) * wide(inv[b], width)).astype(jnp.bfloat16)
            locals_[c][b] = z
            groups[c][pl.ds(b * per, per)] = z.reshape(per, 16, width)
            exts[c][b] = z
            return carry

        lax.fori_loop(0, blocks, one, 0, unroll=UNROLL)

    for copy in small + [load_features, load_embeddings]:
        copy.wait()
    for copy in late:
        copy.start()

    for c in range(chunks):
        with jax.named_scope("prepare"):
            prepare(c)
            stage_hubs(c)
            stage_rims(c)
        if c == 0:
            with jax.named_scope("barrier"):
                pl.semaphore_wait(barrier, n - 1 - jnp.where(head, quarter, 0))
        with jax.named_scope("launch"):
            launch_first(c)
            launch_rims(c)
    with jax.named_scope("weights"):
        for copy in late:
            copy.wait()
        weight[...] = weight_t[...].T

    @pl.when(third)
    def _():
        with jax.named_scope("pass"):
            for c in range(chunks):
                pass_on(c, 1)
                pass_on(c, 0)

    for hop in range(HOPS):
        for c in range(chunks):
            i = hop * chunks + c
            j = i + chunks
            which, at, width = pieces[c]
            with jax.named_scope(f"hubwait_{hop}_{c}"):
                if hop:
                    hub_wait(i, hub_recv_sem.at[i % (2 * chunks)])
                else:
                    first_wait(c, hub_recv_sem.at[c], n - 1, n - 3)
            with jax.named_scope(f"rimwait_{hop}_{c}"):
                rim_wait(i, rim_recv_sem.at[i % (2 * chunks)])

            if i == pairs - 1:
                continue

            hubs = hub_bufs[i][:n].reshape(n * hub_dev, width)

            def one(b, carry):
                rows = pl.ds(pl.multiple_of(b * tile, tile), tile)
                y = gathered(b, rows, taps, tiles, weight, cols_ref, exts[i], hubs)
                root = wide(inv[b], width)
                x = (y * root).astype(jnp.bfloat16)
                (out_f, out_e)[which][hop, rows, at : at + width] = x
                if hop + 1 < HOPS:
                    z = (x.astype(jnp.float32) * root).astype(jnp.bfloat16)
                    locals_[j][b] = z
                    groups[j][pl.ds(b * per, per)] = z.reshape(per, 16, width)
                    exts[j][b] = z
                return carry

            with jax.named_scope(f"compute_{hop}_{c}"):
                lax.fori_loop(0, blocks, one, 0, unroll=UNROLL)
            if hop + 1 < HOPS:
                with jax.named_scope(f"launch_{hop}_{c}"):
                    stage_hubs(j)
                    if hop:
                        hub_wait(i, hub_send_sem.at[c])
                    else:
                        first_wait(c, hub_send_sem.at[c], n - 1 - quarter, n - 1 + 2 * quarter)
                    launch_hubs(j)
                    stage_rims(j)
                    rim_wait(i, rim_send_sem.at[c])
                    launch_rims(j)

    with jax.named_scope("drain"):
        for i in range(pairs - chunks, pairs):
            hub_wait(i, hub_send_sem.at[i % chunks])
            rim_wait(i, rim_send_sem.at[i % chunks])


def flush(
    n, sizes, held_f, held_e, tiles, weight, inv, ext, hubs_ref, cols_hbm,
    out_f, out_e, cols, held, sem,
):
    blocks, tile, taps, send_most, hub_dev, pieces = sizes
    _, at, width = pieces[-1]
    last = HOPS - 1
    fetch = pltpu.make_async_copy(cols_hbm, cols, sem.at[0])
    fetch.start()
    copies = [
        pltpu.make_async_copy(held_f, out_f, sem.at[1]),
        pltpu.make_async_copy(held_e.at[:last], out_e.at[:last], sem.at[2]),
    ]
    if at:
        done = pl.ds(0, at)
        copies.append(pltpu.make_async_copy(held_e.at[last, :, done], out_e.at[last, :, done], sem.at[3]))
    for copy in copies:
        copy.start()
    fetch.wait()
    hubs = hubs_ref[:n].reshape(n * hub_dev, width)

    def one(b, carry):
        rows = pl.ds(pl.multiple_of(b * tile, tile), tile)
        y = gathered(b, rows, taps, tiles, weight, cols, ext, hubs)
        held[rows, :] = (y * wide(inv[b], width)).astype(jnp.bfloat16)
        return carry

    lax.fori_loop(0, blocks, one, 0, unroll=UNROLL)
    rest = pltpu.make_async_copy(held, out_e.at[last, :, pl.ds(at, width)], sem.at[4])
    rest.start()
    for copy in copies + [rest]:
        copy.wait()


def body(
    features, embeddings, tile_values, tile_columns, send_blocks, send_count,
    hub_rows, hub_weight, degree,
):
    n = lax.axis_size("dom")
    rows = features.shape[0]
    blocks, taps, tile, _ = tile_values.shape
    send_most = send_blocks.shape[2]
    hub_dev = hub_rows.shape[0]
    pieces = cut(0, features.shape[1]) + cut(1, embeddings.shape[1])
    sizes = (blocks, tile, taps, send_most, hub_dev, pieces)
    widths = [width for _, _, width in pieces] * HOPS
    vmem = pl.BlockSpec(memory_space=pltpu.VMEM)
    hbm = pl.BlockSpec(memory_space=pltpu.HBM)
    bf16 = jnp.bfloat16
    results = [
        ((HOPS, rows, features.shape[1]), bf16),
        ((HOPS, rows, embeddings.shape[1]), bf16),
        (tile_values.shape, bf16),
        ((rows, n * hub_dev), bf16),
        ((blocks, tile, LANES), jnp.float32),
        ((blocks + 2 * send_most, tile, widths[-1]), bf16),
        ((n + n // 2, hub_dev, widths[-1]), bf16),
    ]
    out_bytes = sum(math.prod(shape[:-1]) * max(shape[-1], LANES) * jnp.dtype(kind).itemsize for shape, kind in results)
    columns = tile_columns.T
    held = pl.pallas_call(
        functools.partial(kernel, n, sizes),
        out_shape=tuple(pltpu.VMEM(shape, kind) for shape, kind in results),
        in_specs=[hbm] * 9,
        out_specs=(vmem,) * len(results),
        scratch_shapes=[
            pltpu.VMEM(shape + (width,), bf16)
            for shape, some in (
                ((blocks, tile), widths),
                ((rows // 16, 16), widths),
                ((2, send_most, tile), widths),
                ((hub_dev,), widths),
                ((blocks + 2 * send_most, tile), widths[:-1]),
                ((n + n // 2, hub_dev), widths[:-1]),
            )
            for width in some
        ]
        + [
            pltpu.SMEM((taps, blocks), jnp.int32),
            pltpu.SMEM(send_blocks.shape, jnp.int32),
            pltpu.SMEM(send_count.shape, jnp.int32),
            pltpu.SMEM(hub_rows.shape, jnp.int32),
            pltpu.VMEM(features.shape, bf16),
            pltpu.VMEM(embeddings.shape, bf16),
            pltpu.VMEM((n * hub_dev, rows), bf16),
            pltpu.VMEM((blocks, tile), jnp.int32),
            pltpu.SemaphoreType.DMA((6,)),
            pltpu.SemaphoreType.DMA((len(pieces),)),
            pltpu.SemaphoreType.DMA((2 * len(pieces),)),
            pltpu.SemaphoreType.DMA((len(pieces),)),
            pltpu.SemaphoreType.DMA((2 * len(pieces),)),
            pltpu.SemaphoreType.DMA((len(pieces), 2)),
        ],
        compiler_params=pltpu.CompilerParams(
            collective_id=0, has_side_effects=True, vmem_limit_bytes=VMEM - out_bytes
        ),
    )(
        columns, send_blocks, send_count, hub_rows,
        features, embeddings, tile_values, hub_weight.T,
        degree.reshape(blocks, tile),
    )
    return pl.pallas_call(
        functools.partial(flush, n, sizes),
        out_shape=tuple(jax.ShapeDtypeStruct(h.shape, h.dtype) for h in held[:2]),
        in_specs=[vmem] * len(held) + [hbm],
        out_specs=(hbm, hbm),
        scratch_shapes=[
            pltpu.SMEM((taps, blocks), jnp.int32),
            pltpu.VMEM((rows, widths[-1]), bf16),
            pltpu.SemaphoreType.DMA((5,)),
        ],
        compiler_params=pltpu.CompilerParams(vmem_limit_bytes=4 * 2**20),
    )(*held, columns)


def solution(mesh):
    placed = (
        P("dom", None),
        P("dom", None),
        P("dom", None, None, None),
        P("dom", None),
        P("dom", None, None),
        P("dom", None),
        P("dom"),
        P("dom", None),
        P("dom"),
    )
    return jax.shard_map(
        body,
        mesh=mesh,
        in_specs=placed,
        out_specs=(P(None, "dom", None), P(None, "dom", None)),
        check_vma=False,
    )
```

```python
import functools
import math

import jax
import jax.numpy as jnp
from jax import lax
from jax.experimental import pallas as pl
from jax.experimental.pallas import tpu as pltpu
from jax.sharding import PartitionSpec as P

HOPS = 3
LANES = 128
WIDTH = 256
UNROLL = 4
VMEM = 67043328
MESH = pl.DeviceIdType.MESH


def cut(which, columns):
    return [(which, at, min(WIDTH, columns - at)) for at in range(0, columns, WIDTH)]


def wide(root, width):
    return jnp.concatenate([root] * (width // LANES), axis=1)


def gathered(b, rows, taps, tiles, weight, cols, ext, hubs):
    left = jnp.concatenate([tiles[b, k] for k in range(taps)], axis=1)
    right = jnp.concatenate([ext[cols[k, b]] for k in range(taps)], axis=0)
    y = jnp.dot(left, right, preferred_element_type=jnp.float32)
    return y + jnp.dot(weight[rows, :], hubs, preferred_element_type=jnp.float32)


def kernel(
    n, sizes, cols_hbm, listed_hbm, count_hbm, hubs_hbm,
    features_hbm, embeddings_hbm, tiles_hbm, weight_hbm, degree_hbm,
    out_f, out_e, tiles, weight, inv, last_ext, last_hubs, cols_held, *scratch,
):
    blocks, tile, taps, send_most, hub_dev, pieces = sizes
    chunks = len(pieces)
    per = tile // 16
    pairs = HOPS * chunks
    scratch = list(scratch)
    take = lambda count: [scratch.pop(0) for _ in range(count)]
    locals_, groups, sends, hub_sends = (take(pairs) for _ in range(4))
    exts = take(pairs - 1) + [last_ext]
    hub_bufs = take(pairs - 1) + [last_hubs]
    (
        cols_ref, listed_ref, count_ref, hubs_ref,
        features, embeddings, weight_t, degree,
        load_sem, rim_send_sem, rim_recv_sem, hub_send_sem, hub_recv_sem, pass_sem,
    ) = scratch
    me = lax.axis_index("dom")

    def load(source, held, q):
        return pltpu.make_async_copy(source, held, load_sem.at[q])

    load_degree = load(degree_hbm, degree, 0)
    load_features = load(features_hbm, features, 1)
    load_embeddings = load(embeddings_hbm, embeddings, 2)
    small = [
        load(listed_hbm, listed_ref, 3),
        load(count_hbm, count_ref, 4),
        load(hubs_hbm, hubs_ref, 5),
    ]
    late = [
        load(tiles_hbm, tiles, 0),
        load(weight_hbm, weight_t, 1),
        load(cols_hbm, cols_ref, 2),
        load(cols_hbm, cols_held, 3),
    ]
    for copy in [load_degree, load_features, load_embeddings] + small:
        copy.start()

    barrier = pltpu.get_barrier_semaphore()

    quarter = n // 4
    head = me < 2 * quarter
    third = jnp.logical_and(me >= 2 * quarter, me < 3 * quarter)
    tail = me >= 3 * quarter

    def greet(step, carry):
        to = lax.rem(me + step, n)

        @pl.when(jnp.logical_not(jnp.logical_and(tail, to < 2 * quarter)))
        def _():
            pl.semaphore_signal(barrier, inc=1, device_id=(to,), device_id_type=MESH)

        return carry

    lax.fori_loop(1, n, greet, 0)

    @pl.when(me == 0)
    def _():
        for i in range(pairs):
            exts[i][blocks : blocks + send_most] = jnp.zeros((send_most,) + exts[i].shape[1:], jnp.bfloat16)

    @pl.when(me == n - 1)
    def _():
        for i in range(pairs):
            exts[i][blocks + send_most :] = jnp.zeros((send_most,) + exts[i].shape[1:], jnp.bfloat16)

    load_degree.wait()
    roots = lax.rsqrt(degree[...].astype(jnp.float32)).T
    for b in range(blocks):
        inv[b] = jnp.broadcast_to(roots[:, b : b + 1], (tile, LANES))

    def rim_copy(i, side):
        first = blocks if side == 1 else blocks + send_most
        to = me + 1 if side == 1 else me - 1
        return pltpu.make_async_remote_copy(
            src_ref=sends[i].at[side],
            dst_ref=exts[i].at[pl.ds(first, send_most)],
            send_sem=rim_send_sem.at[i % chunks],
            recv_sem=rim_recv_sem.at[i % (2 * chunks)],
            device_id=(to,),
            device_id_type=MESH,
        )

    inner = jnp.logical_and(me > 0, me < n - 1)

    def rim_wait(i, sem):
        def of(count):
            some = exts[i].at[pl.ds(blocks, count)]
            return pltpu.make_async_copy(some, some, sem)

        @pl.when(inner)
        def _():
            of(2 * send_most).wait()

        @pl.when(jnp.logical_not(inner))
        def _():
            of(send_most).wait()

    def hub_wait(i, sem, count=n - 1):
        some = hub_bufs[i].at[pl.ds(0, count)]
        pltpu.make_async_copy(some, some, sem).wait()

    def hub_copy(i, held, owner, to, recv_sem):
        return pltpu.make_async_remote_copy(
            src_ref=held,
            dst_ref=hub_bufs[i].at[owner],
            send_sem=hub_send_sem.at[i % chunks],
            recv_sem=recv_sem,
            device_id=(to,),
            device_id_type=MESH,
        )

    def row_of(rows, row):
        here = lax.broadcasted_iota(jnp.int32, rows.shape, 0) == lax.rem(row, 16)
        return jnp.sum(jnp.where(here, rows.astype(jnp.float32), 0.0), axis=0, keepdims=True)

    def stage_rims(i):
        for side in range(2):
            for s in range(send_most):
                block = locals_[i][listed_ref[0, side, s]]
                keep = jnp.where(s < count_ref[0, side], 1.0, 0.0).astype(jnp.float32)
                sends[i][side, s] = (block.astype(jnp.float32) * keep).astype(jnp.bfloat16)

    def stage_hubs(i):
        near = [groups[i][lax.div(hubs_ref[q], 16)] for q in range(hub_dev)]
        picked = [row_of(near[q], hubs_ref[q]) for q in range(hub_dev)]
        packed = jnp.concatenate(picked, axis=0).astype(jnp.bfloat16)
        hub_sends[i][...] = packed
        hub_bufs[i][me] = packed

    def launch_rims(i):
        @pl.when(me < n - 1)
        def _():
            rim_copy(i, 1).start()

        @pl.when(me > 0)
        def _():
            rim_copy(i, 0).start()

    def launch_hubs(i):
        recv_sem = hub_recv_sem.at[i % (2 * chunks)]

        def spread(step, carry):
            hub_copy(i, hub_sends[i], me, lax.rem(me + step, n), recv_sem).start()
            return carry

        lax.fori_loop(1, n, spread, 0)

    def launch_first(c):
        recv_sem = hub_recv_sem.at[c]

        def spread(step, carry):
            hub_copy(c, hub_sends[c], me, lax.rem(me + step, n), recv_sem).start()
            return carry

        @pl.when(head)
        def _():
            source = lax.div(me, quarter)
            passer = me + (2 - source) * quarter
            hub_copy(c, hub_sends[c], me, passer, pass_sem.at[c, source]).start()

            def near(step, carry):
                to = lax.rem(me + step, 3 * quarter)

                @pl.when(to != passer)
                def _():
                    hub_copy(c, hub_sends[c], me, to, recv_sem).start()

                return carry

            lax.fori_loop(1, 3 * quarter, near, 0)

        @pl.when(jnp.logical_not(head))
        def _():
            lax.fori_loop(1, n, spread, 0)

    def pass_on(c, source):
        owner = me - (2 - source) * quarter
        hub_wait(c, pass_sem.at[c, source], 1)

        def spread(step, carry):
            to = 3 * quarter + lax.rem(me + step, quarter)
            hub_copy(c, hub_bufs[c].at[owner], owner, to, hub_recv_sem.at[c]).start()
            return carry

        lax.fori_loop(0, quarter, spread, 0)

    def first_wait(c, sem, of_head, of_third):
        @pl.when(head)
        def _():
            hub_wait(c, sem, of_head)

        @pl.when(third)
        def _():
            hub_wait(c, sem, of_third)

        @pl.when(tail)
        def _():
            hub_wait(c, sem)

    def prepare(c):
        which, at, width = pieces[c]

        def one(b, carry):
            rows = pl.ds(pl.multiple_of(b * tile, tile), tile)
            x = (features, embeddings)[which][rows, at : at + width]
            z = (x.astype(jnp.float32) * wide(inv[b], width)).astype(jnp.bfloat16)
            locals_[c][b] = z
            groups[c][pl.ds(b * per, per)] = z.reshape(per, 16, width)
            exts[c][b] = z
            return carry

        lax.fori_loop(0, blocks, one, 0, unroll=UNROLL)

    for copy in small + [load_features, load_embeddings]:
        copy.wait()
    for copy in late:
        copy.start()

    for c in range(chunks):
        with jax.named_scope("prepare"):
            prepare(c)
            stage_hubs(c)
            stage_rims(c)
        if c == 0:
            with jax.named_scope("barrier"):
                pl.semaphore_wait(barrier, n - 1 - jnp.where(head, quarter, 0))
        with jax.named_scope("launch"):
            launch_first(c)
            launch_rims(c)
    with jax.named_scope("weights"):
        for copy in late:
            copy.wait()
        weight[...] = weight_t[...].T

    @pl.when(third)
    def _():
        with jax.named_scope("pass"):
            for c in range(chunks):
                pass_on(c, 1)
                pass_on(c, 0)

    for hop in range(HOPS):
        for c in range(chunks):
            i = hop * chunks + c
            j = i + chunks
            which, at, width = pieces[c]
            with jax.named_scope(f"hubwait_{hop}_{c}"):
                if hop:
                    hub_wait(i, hub_recv_sem.at[i % (2 * chunks)])
                else:
                    first_wait(c, hub_recv_sem.at[c], n - 1, n - 3)
            with jax.named_scope(f"rimwait_{hop}_{c}"):
                rim_wait(i, rim_recv_sem.at[i % (2 * chunks)])

            if i == pairs - 1:
                continue

            hubs = hub_bufs[i][:n].reshape(n * hub_dev, width)

            def one(b, carry):
                rows = pl.ds(pl.multiple_of(b * tile, tile), tile)
                y = gathered(b, rows, taps, tiles, weight, cols_ref, exts[i], hubs)
                root = wide(inv[b], width)
                x = (y * root).astype(jnp.bfloat16)
                (out_f, out_e)[which][hop, rows, at : at + width] = x
                if hop + 1 < HOPS:
                    z = (x.astype(jnp.float32) * root).astype(jnp.bfloat16)
                    locals_[j][b] = z
                    groups[j][pl.ds(b * per, per)] = z.reshape(per, 16, width)
                    exts[j][b] = z
                return carry

            with jax.named_scope(f"compute_{hop}_{c}"):
                lax.fori_loop(0, blocks, one, 0, unroll=UNROLL)
            if hop + 1 < HOPS:
                with jax.named_scope(f"launch_{hop}_{c}"):
                    stage_hubs(j)
                    if hop:
                        hub_wait(i, hub_send_sem.at[c])
                    else:
                        first_wait(c, hub_send_sem.at[c], n - 1 - quarter, n - 1 + 2 * quarter)
                    launch_hubs(j)
                    stage_rims(j)
                    rim_wait(i, rim_send_sem.at[c])
                    launch_rims(j)

    with jax.named_scope("drain"):
        for i in range(pairs - chunks, pairs):
            hub_wait(i, hub_send_sem.at[i % chunks])
            rim_wait(i, rim_send_sem.at[i % chunks])


def flush(
    n, sizes, held_f, held_e, tiles, weight, inv, ext, hubs_ref, cols_held,
    out_f, out_e, cols, held, sem,
):
    blocks, tile, taps, send_most, hub_dev, pieces = sizes
    _, at, width = pieces[-1]
    last = HOPS - 1
    fetch = pltpu.make_async_copy(cols_held, cols, sem.at[0])
    fetch.start()
    copies = [
        pltpu.make_async_copy(held_f, out_f, sem.at[1]),
        pltpu.make_async_copy(held_e.at[:last], out_e.at[:last], sem.at[2]),
    ]
    if at:
        done = pl.ds(0, at)
        copies.append(pltpu.make_async_copy(held_e.at[last, :, done], out_e.at[last, :, done], sem.at[3]))
    for copy in copies:
        copy.start()
    fetch.wait()
    hubs = hubs_ref[:n].reshape(n * hub_dev, width)

    def one(b, carry):
        rows = pl.ds(pl.multiple_of(b * tile, tile), tile)
        y = gathered(b, rows, taps, tiles, weight, cols, ext, hubs)
        held[rows, :] = (y * wide(inv[b], width)).astype(jnp.bfloat16)
        return carry

    lax.fori_loop(0, blocks, one, 0, unroll=UNROLL)
    rest = pltpu.make_async_copy(held, out_e.at[last, :, pl.ds(at, width)], sem.at[4])
    rest.start()
    for copy in copies + [rest]:
        copy.wait()


def body(
    features, embeddings, tile_values, tile_columns, send_blocks, send_count,
    hub_rows, hub_weight, degree,
):
    n = lax.axis_size("dom")
    rows = features.shape[0]
    blocks, taps, tile, _ = tile_values.shape
    send_most = send_blocks.shape[2]
    hub_dev = hub_rows.shape[0]
    pieces = cut(0, features.shape[1]) + cut(1, embeddings.shape[1])
    sizes = (blocks, tile, taps, send_most, hub_dev, pieces)
    widths = [width for _, _, width in pieces] * HOPS
    vmem = pl.BlockSpec(memory_space=pltpu.VMEM)
    hbm = pl.BlockSpec(memory_space=pltpu.HBM)
    bf16 = jnp.bfloat16
    results = [
        ((HOPS, rows, features.shape[1]), bf16),
        ((HOPS, rows, embeddings.shape[1]), bf16),
        (tile_values.shape, bf16),
        ((rows, n * hub_dev), bf16),
        ((blocks, tile, LANES), jnp.float32),
        ((blocks + 2 * send_most, tile, widths[-1]), bf16),
        ((n + n // 2, hub_dev, widths[-1]), bf16),
        ((taps, blocks), jnp.int32),
    ]
    out_bytes = sum(math.prod(shape[:-1]) * max(shape[-1], LANES) * jnp.dtype(kind).itemsize for shape, kind in results)
    held = pl.pallas_call(
        functools.partial(kernel, n, sizes),
        out_shape=tuple(pltpu.VMEM(shape, kind) for shape, kind in results),
        in_specs=[hbm] * 9,
        out_specs=(vmem,) * len(results),
        scratch_shapes=[
            pltpu.VMEM(shape + (width,), bf16)
            for shape, some in (
                ((blocks, tile), widths),
                ((rows // 16, 16), widths),
                ((2, send_most, tile), widths),
                ((hub_dev,), widths),
                ((blocks + 2 * send_most, tile), widths[:-1]),
                ((n + n // 2, hub_dev), widths[:-1]),
            )
            for width in some
        ]
        + [
            pltpu.SMEM((taps, blocks), jnp.int32),
            pltpu.SMEM(send_blocks.shape, jnp.int32),
            pltpu.SMEM(send_count.shape, jnp.int32),
            pltpu.SMEM(hub_rows.shape, jnp.int32),
            pltpu.VMEM(features.shape, bf16),
            pltpu.VMEM(embeddings.shape, bf16),
            pltpu.VMEM((n * hub_dev, rows), bf16),
            pltpu.VMEM((blocks, tile), jnp.int32),
            pltpu.SemaphoreType.DMA((6,)),
            pltpu.SemaphoreType.DMA((len(pieces),)),
            pltpu.SemaphoreType.DMA((2 * len(pieces),)),
            pltpu.SemaphoreType.DMA((len(pieces),)),
            pltpu.SemaphoreType.DMA((2 * len(pieces),)),
            pltpu.SemaphoreType.DMA((len(pieces), 2)),
        ],
        compiler_params=pltpu.CompilerParams(
            collective_id=0, has_side_effects=True, vmem_limit_bytes=VMEM - out_bytes - 2**20
        ),
    )(
        tile_columns.T, send_blocks, send_count, hub_rows,
        features, embeddings, tile_values, hub_weight.T,
        degree.reshape(blocks, tile),
    )
    return pl.pallas_call(
        functools.partial(flush, n, sizes),
        out_shape=tuple(jax.ShapeDtypeStruct(h.shape, h.dtype) for h in held[:2]),
        in_specs=[vmem] * len(held),
        out_specs=(hbm, hbm),
        scratch_shapes=[
            pltpu.SMEM((taps, blocks), jnp.int32),
            pltpu.VMEM((rows, widths[-1]), bf16),
            pltpu.SemaphoreType.DMA((5,)),
        ],
        compiler_params=pltpu.CompilerParams(vmem_limit_bytes=4 * 2**20),
    )(*held)


def solution(mesh):
    placed = (
        P("dom", None),
        P("dom", None),
        P("dom", None, None, None),
        P("dom", None),
        P("dom", None, None),
        P("dom", None),
        P("dom"),
        P("dom", None),
        P("dom"),
    )
    return jax.shard_map(
        body,
        mesh=mesh,
        in_specs=placed,
        out_specs=(P(None, "dom", None), P(None, "dom", None)),
        check_vma=False,
    )
```

```python
import functools
import math

import jax
import jax.numpy as jnp
from jax import lax
from jax.experimental import pallas as pl
from jax.experimental.pallas import tpu as pltpu
from jax.sharding import PartitionSpec as P

HOPS = 3
LANES = 128
WIDTH = 128
UNROLL = 4
VMEM = 67043328
MESH = pl.DeviceIdType.MESH


def cut(which, columns):
    return [(which, at, min(WIDTH, columns - at)) for at in range(0, columns, WIDTH)]


def wide(root, width):
    return jnp.concatenate([root] * (width // LANES), axis=1)


def gathered(b, rows, taps, tiles, weight, cols, ext, hubs):
    left = jnp.concatenate([tiles[b, k] for k in range(taps)], axis=1)
    right = jnp.concatenate([ext[cols[k, b]] for k in range(taps)], axis=0)
    y = jnp.dot(left, right, preferred_element_type=jnp.float32)
    return y + jnp.dot(weight[rows, :], hubs, preferred_element_type=jnp.float32)


def kernel(
    n, sizes, cols_hbm, listed_hbm, count_hbm, hubs_hbm,
    features_hbm, embeddings_hbm, tiles_hbm, weight_hbm, degree_hbm,
    out_f, out_e, tiles, weight, inv, last_ext, last_hubs, cols_held, *scratch,
):
    blocks, tile, taps, send_most, hub_dev, pieces = sizes
    chunks = len(pieces)
    per = tile // 16
    pairs = HOPS * chunks
    scratch = list(scratch)
    take = lambda count: [scratch.pop(0) for _ in range(count)]
    locals_, groups, sends, hub_sends = (take(pairs) for _ in range(4))
    exts = take(pairs - 1) + [last_ext]
    hub_bufs = take(pairs - 1) + [last_hubs]
    (
        cols_ref, listed_ref, count_ref, hubs_ref,
        features, embeddings, weight_t, degree,
        load_sem, rim_send_sem, rim_recv_sem, hub_send_sem, hub_recv_sem, pass_sem,
    ) = scratch
    me = lax.axis_index("dom")

    def load(source, held, q):
        return pltpu.make_async_copy(source, held, load_sem.at[q])

    load_degree = load(degree_hbm, degree, 0)
    load_features = load(features_hbm, features, 1)
    load_embeddings = load(embeddings_hbm, embeddings, 2)
    small = [
        load(listed_hbm, listed_ref, 3),
        load(count_hbm, count_ref, 4),
        load(hubs_hbm, hubs_ref, 5),
    ]
    late = [
        load(tiles_hbm, tiles, 0),
        load(weight_hbm, weight_t, 1),
        load(cols_hbm, cols_ref, 2),
        load(cols_hbm, cols_held, 3),
    ]
    for copy in [load_degree, load_features, load_embeddings]:
        copy.start()

    barrier = pltpu.get_barrier_semaphore()

    quarter = n // 4
    head = me < 2 * quarter
    third = jnp.logical_and(me >= 2 * quarter, me < 3 * quarter)
    tail = me >= 3 * quarter

    def greet(to, carry):
        @pl.when(to != me)
        def _():
            pl.semaphore_signal(barrier, inc=1, device_id=(to,), device_id_type=MESH)

        return carry

    lax.fori_loop(jnp.where(tail, 2 * quarter, 0), n, greet, 0)
    for copy in small:
        copy.start()

    @pl.when(me == 0)
    def _():
        for i in range(pairs):
            exts[i][blocks : blocks + send_most] = jnp.zeros((send_most,) + exts[i].shape[1:], jnp.bfloat16)

    @pl.when(me == n - 1)
    def _():
        for i in range(pairs):
            exts[i][blocks + send_most :] = jnp.zeros((send_most,) + exts[i].shape[1:], jnp.bfloat16)

    load_degree.wait()
    roots = lax.rsqrt(degree[...].astype(jnp.float32)).T
    for b in range(blocks):
        inv[b] = jnp.broadcast_to(roots[:, b : b + 1], (tile, LANES))

    def rim_copy(i, side):
        first = blocks if side == 1 else blocks + send_most
        to = me + 1 if side == 1 else me - 1
        return pltpu.make_async_remote_copy(
            src_ref=sends[i].at[side],
            dst_ref=exts[i].at[pl.ds(first, send_most)],
            send_sem=rim_send_sem.at[i % chunks],
            recv_sem=rim_recv_sem.at[i % (2 * chunks)],
            device_id=(to,),
            device_id_type=MESH,
        )

    inner = jnp.logical_and(me > 0, me < n - 1)

    def rim_wait(i, sem):
        def of(count):
            some = exts[i].at[pl.ds(blocks, count)]
            return pltpu.make_async_copy(some, some, sem)

        @pl.when(inner)
        def _():
            of(2 * send_most).wait()

        @pl.when(jnp.logical_not(inner))
        def _():
            of(send_most).wait()

    def hub_wait(i, sem, count=n - 1):
        some = hub_bufs[i].at[pl.ds(0, count)]
        pltpu.make_async_copy(some, some, sem).wait()

    def hub_copy(i, held, owner, to, recv_sem):
        return pltpu.make_async_remote_copy(
            src_ref=held,
            dst_ref=hub_bufs[i].at[owner],
            send_sem=hub_send_sem.at[i % chunks],
            recv_sem=recv_sem,
            device_id=(to,),
            device_id_type=MESH,
        )

    def row_of(rows, row):
        here = lax.broadcasted_iota(jnp.int32, rows.shape, 0) == lax.rem(row, 16)
        return jnp.sum(jnp.where(here, rows.astype(jnp.float32), 0.0), axis=0, keepdims=True)

    def stage_rims(i):
        for side in range(2):
            for s in range(send_most):
                block = locals_[i][listed_ref[0, side, s]]
                keep = jnp.where(s < count_ref[0, side], 1.0, 0.0).astype(jnp.float32)
                sends[i][side, s] = (block.astype(jnp.float32) * keep).astype(jnp.bfloat16)

    def stage_hubs(i):
        near = [groups[i][lax.div(hubs_ref[q], 16)] for q in range(hub_dev)]
        picked = [row_of(near[q], hubs_ref[q]) for q in range(hub_dev)]
        packed = jnp.concatenate(picked, axis=0).astype(jnp.bfloat16)
        hub_sends[i][...] = packed
        hub_bufs[i][me] = packed

    def launch_rims(i):
        @pl.when(me < n - 1)
        def _():
            rim_copy(i, 1).start()

        @pl.when(me > 0)
        def _():
            rim_copy(i, 0).start()

    def launch_hubs(i):
        recv_sem = hub_recv_sem.at[i % (2 * chunks)]

        def spread(step, carry):
            hub_copy(i, hub_sends[i], me, lax.rem(me + step, n), recv_sem).start()
            return carry

        lax.fori_loop(1, n, spread, 0)

    def launch_first(c):
        recv_sem = hub_recv_sem.at[c]

        def spread(step, carry):
            hub_copy(c, hub_sends[c], me, lax.rem(me + step, n), recv_sem).start()
            return carry

        @pl.when(head)
        def _():
            source = lax.div(me, quarter)
            passer = me + (2 - source) * quarter
            hub_copy(c, hub_sends[c], me, passer, pass_sem.at[c, source]).start()

            def near(step, carry):
                to = lax.rem(me + step, 3 * quarter)

                @pl.when(to != passer)
                def _():
                    hub_copy(c, hub_sends[c], me, to, recv_sem).start()

                return carry

            lax.fori_loop(1, 3 * quarter, near, 0)

        @pl.when(jnp.logical_not(head))
        def _():
            lax.fori_loop(1, n, spread, 0)

    def pass_on(c, source):
        owner = me - (2 - source) * quarter
        hub_wait(c, pass_sem.at[c, source], 1)

        def spread(step, carry):
            to = 3 * quarter + lax.rem(me + step, quarter)
            hub_copy(c, hub_bufs[c].at[owner], owner, to, hub_recv_sem.at[c]).start()
            return carry

        lax.fori_loop(0, quarter, spread, 0)

    def first_wait(c, sem, of_head, of_third):
        @pl.when(head)
        def _():
            hub_wait(c, sem, of_head)

        @pl.when(third)
        def _():
            hub_wait(c, sem, of_third)

        @pl.when(tail)
        def _():
            hub_wait(c, sem)

    def prepare(c):
        which, at, width = pieces[c]

        def one(b, carry):
            rows = pl.ds(pl.multiple_of(b * tile, tile), tile)
            x = (features, embeddings)[which][rows, at : at + width]
            z = (x.astype(jnp.float32) * wide(inv[b], width)).astype(jnp.bfloat16)
            locals_[c][b] = z
            groups[c][pl.ds(b * per, per)] = z.reshape(per, 16, width)
            exts[c][b] = z
            return carry

        lax.fori_loop(0, blocks, one, 0, unroll=UNROLL)

    for copy in small + [load_features, load_embeddings]:
        copy.wait()
    for copy in late:
        copy.start()

    for c in range(chunks):
        with jax.named_scope("prepare"):
            prepare(c)
            stage_hubs(c)
            stage_rims(c)
        if c == 0:
            with jax.named_scope("barrier"):
                pl.semaphore_wait(barrier, n - 1 - jnp.where(head, quarter, 0))
        with jax.named_scope("launch"):
            launch_first(c)
            launch_rims(c)
    with jax.named_scope("weights"):
        for copy in late:
            copy.wait()
        weight[...] = weight_t[...].T

    @pl.when(third)
    def _():
        with jax.named_scope("pass"):
            for c in range(chunks):
                pass_on(c, 1)
                pass_on(c, 0)

    for hop in range(HOPS):
        for c in range(chunks):
            i = hop * chunks + c
            j = i + chunks
            which, at, width = pieces[c]
            with jax.named_scope(f"hubwait_{hop}_{c}"):
                if hop:
                    hub_wait(i, hub_recv_sem.at[i % (2 * chunks)])
                else:
                    first_wait(c, hub_recv_sem.at[c], n - 1, n - 3)
            with jax.named_scope(f"rimwait_{hop}_{c}"):
                rim_wait(i, rim_recv_sem.at[i % (2 * chunks)])

            if i == pairs - 1:
                continue

            hubs = hub_bufs[i][:n].reshape(n * hub_dev, width)

            def one(b, carry):
                rows = pl.ds(pl.multiple_of(b * tile, tile), tile)
                y = gathered(b, rows, taps, tiles, weight, cols_ref, exts[i], hubs)
                root = wide(inv[b], width)
                x = (y * root).astype(jnp.bfloat16)
                (out_f, out_e)[which][hop, rows, at : at + width] = x
                if hop + 1 < HOPS:
                    z = (x.astype(jnp.float32) * root).astype(jnp.bfloat16)
                    locals_[j][b] = z
                    groups[j][pl.ds(b * per, per)] = z.reshape(per, 16, width)
                    exts[j][b] = z
                return carry

            with jax.named_scope(f"compute_{hop}_{c}"):
                lax.fori_loop(0, blocks, one, 0, unroll=UNROLL)
            if hop + 1 < HOPS:
                with jax.named_scope(f"launch_{hop}_{c}"):
                    stage_hubs(j)
                    if hop:
                        hub_wait(i, hub_send_sem.at[c])
                    else:
                        first_wait(c, hub_send_sem.at[c], n - 1 - quarter, n - 1 + 2 * quarter)
                    launch_hubs(j)
                    stage_rims(j)
                    rim_wait(i, rim_send_sem.at[c])
                    launch_rims(j)

    with jax.named_scope("drain"):
        for i in range(pairs - chunks, pairs):
            hub_wait(i, hub_send_sem.at[i % chunks])
            rim_wait(i, rim_send_sem.at[i % chunks])


def flush(
    n, sizes, held_f, held_e, tiles, weight, inv, ext, hubs_ref, cols_held,
    out_f, out_e, cols, held, sem,
):
    blocks, tile, taps, send_most, hub_dev, pieces = sizes
    _, at, width = pieces[-1]
    last = HOPS - 1
    fetch = pltpu.make_async_copy(cols_held, cols, sem.at[0])
    fetch.start()
    copies = [
        pltpu.make_async_copy(held_f, out_f, sem.at[1]),
        pltpu.make_async_copy(held_e.at[:last], out_e.at[:last], sem.at[2]),
    ]
    if at:
        done = pl.ds(0, at)
        copies.append(pltpu.make_async_copy(held_e.at[last, :, done], out_e.at[last, :, done], sem.at[3]))
    for copy in copies:
        copy.start()
    fetch.wait()
    hubs = hubs_ref[:n].reshape(n * hub_dev, width)

    def one(b, carry):
        rows = pl.ds(pl.multiple_of(b * tile, tile), tile)
        y = gathered(b, rows, taps, tiles, weight, cols, ext, hubs)
        held[rows, :] = (y * wide(inv[b], width)).astype(jnp.bfloat16)
        return carry

    lax.fori_loop(0, blocks, one, 0, unroll=UNROLL)
    rest = pltpu.make_async_copy(held, out_e.at[last, :, pl.ds(at, width)], sem.at[4])
    rest.start()
    for copy in copies + [rest]:
        copy.wait()


def body(
    features, embeddings, tile_values, tile_columns, send_blocks, send_count,
    hub_rows, hub_weight, degree,
):
    n = lax.axis_size("dom")
    rows = features.shape[0]
    blocks, taps, tile, _ = tile_values.shape
    send_most = send_blocks.shape[2]
    hub_dev = hub_rows.shape[0]
    pieces = cut(0, features.shape[1]) + cut(1, embeddings.shape[1])
    sizes = (blocks, tile, taps, send_most, hub_dev, pieces)
    widths = [width for _, _, width in pieces] * HOPS
    vmem = pl.BlockSpec(memory_space=pltpu.VMEM)
    hbm = pl.BlockSpec(memory_space=pltpu.HBM)
    bf16 = jnp.bfloat16
    results = [
        ((HOPS, rows, features.shape[1]), bf16),
        ((HOPS, rows, embeddings.shape[1]), bf16),
        (tile_values.shape, bf16),
        ((rows, n * hub_dev), bf16),
        ((blocks, tile, LANES), jnp.float32),
        ((blocks + 2 * send_most, tile, widths[-1]), bf16),
        ((n + n // 2, hub_dev, widths[-1]), bf16),
        ((taps, blocks), jnp.int32),
    ]
    out_bytes = sum(math.prod(shape[:-1]) * max(shape[-1], LANES) * jnp.dtype(kind).itemsize for shape, kind in results)
    held = pl.pallas_call(
        functools.partial(kernel, n, sizes),
        out_shape=tuple(pltpu.VMEM(shape, kind) for shape, kind in results),
        in_specs=[hbm] * 9,
        out_specs=(vmem,) * len(results),
        scratch_shapes=[
            pltpu.VMEM(shape + (width,), bf16)
            for shape, some in (
                ((blocks, tile), widths),
                ((rows // 16, 16), widths),
                ((2, send_most, tile), widths),
                ((hub_dev,), widths),
                ((blocks + 2 * send_most, tile), widths[:-1]),
                ((n + n // 2, hub_dev), widths[:-1]),
            )
            for width in some
        ]
        + [
            pltpu.SMEM((taps, blocks), jnp.int32),
            pltpu.SMEM(send_blocks.shape, jnp.int32),
            pltpu.SMEM(send_count.shape, jnp.int32),
            pltpu.SMEM(hub_rows.shape, jnp.int32),
            pltpu.VMEM(features.shape, bf16),
            pltpu.VMEM(embeddings.shape, bf16),
            pltpu.VMEM((n * hub_dev, rows), bf16),
            pltpu.VMEM((blocks, tile), jnp.int32),
            pltpu.SemaphoreType.DMA((6,)),
            pltpu.SemaphoreType.DMA((len(pieces),)),
            pltpu.SemaphoreType.DMA((2 * len(pieces),)),
            pltpu.SemaphoreType.DMA((len(pieces),)),
            pltpu.SemaphoreType.DMA((2 * len(pieces),)),
            pltpu.SemaphoreType.DMA((len(pieces), 2)),
        ],
        compiler_params=pltpu.CompilerParams(
            collective_id=0, has_side_effects=True, vmem_limit_bytes=VMEM - out_bytes - 2**20
        ),
    )(
        tile_columns.T, send_blocks, send_count, hub_rows,
        features, embeddings, tile_values, hub_weight.T,
        degree.reshape(blocks, tile),
    )
    return pl.pallas_call(
        functools.partial(flush, n, sizes),
        out_shape=tuple(jax.ShapeDtypeStruct(h.shape, h.dtype) for h in held[:2]),
        in_specs=[vmem] * len(held),
        out_specs=(hbm, hbm),
        scratch_shapes=[
            pltpu.SMEM((taps, blocks), jnp.int32),
            pltpu.VMEM((rows, widths[-1]), bf16),
            pltpu.SemaphoreType.DMA((5,)),
        ],
        compiler_params=pltpu.CompilerParams(vmem_limit_bytes=4 * 2**20),
    )(*held)


def solution(mesh):
    placed = (
        P("dom", None),
        P("dom", None),
        P("dom", None, None, None),
        P("dom", None),
        P("dom", None, None),
        P("dom", None),
        P("dom"),
        P("dom", None),
        P("dom"),
    )
    return jax.shard_map(
        body,
        mesh=mesh,
        in_specs=placed,
        out_specs=(P(None, "dom", None), P(None, "dom", None)),
        check_vma=False,
    )
```

```python
import functools
import math

import jax
import jax.numpy as jnp
from jax import lax
from jax.experimental import pallas as pl
from jax.experimental.pallas import tpu as pltpu
from jax.sharding import PartitionSpec as P

HOPS = 3
LANES = 128
WIDTH = 128
UNROLL = 4
VMEM = 67043328
MESH = pl.DeviceIdType.MESH


def cut(which, columns):
    return [(which, at, min(WIDTH, columns - at)) for at in range(0, columns, WIDTH)]


def wide(root, width):
    return jnp.concatenate([root] * (width // LANES), axis=1)


def gathered(b, rows, taps, tiles, weight, cols, ext, hubs):
    left = jnp.concatenate([tiles[b, k] for k in range(taps)], axis=1)
    right = jnp.concatenate([ext[cols[k, b]] for k in range(taps)], axis=0)
    y = jnp.dot(left, right, preferred_element_type=jnp.float32)
    return y + jnp.dot(weight[rows, :], hubs, preferred_element_type=jnp.float32)


def kernel(
    n, sizes, cols_hbm, listed_hbm, count_hbm, hubs_hbm,
    features_hbm, embeddings_hbm, tiles_hbm, weight_hbm, degree_hbm,
    out_f, out_e, tiles, weight, inv, last_ext, last_hubs, cols_held, *scratch,
):
    blocks, tile, taps, send_most, hub_dev, pieces = sizes
    chunks = len(pieces)
    per = tile // 16
    pairs = HOPS * chunks
    scratch = list(scratch)
    counted = scratch.pop(0)
    rim_units = send_most * tile // hub_dev
    take = lambda count: [scratch.pop(0) for _ in range(count)]
    locals_, groups, sends, hub_sends = (take(pairs) for _ in range(4))
    exts = take(pairs - 1) + [last_ext]
    hub_bufs = take(pairs - 1) + [last_hubs]
    (
        cols_ref, listed_ref, count_ref, hubs_ref,
        features, embeddings, weight_t, degree,
        load_sem, send_sem, recv_sem, pass_sem,
    ) = scratch
    me = lax.axis_index("dom")

    def load(source, held, q):
        return pltpu.make_async_copy(source, held, load_sem.at[q])

    load_degree = load(degree_hbm, degree, 0)
    load_features = load(features_hbm, features, 1)
    load_embeddings = load(embeddings_hbm, embeddings, 2)
    small = [
        load(listed_hbm, listed_ref, 3),
        load(count_hbm, count_ref, 4),
        load(hubs_hbm, hubs_ref, 5),
    ]
    late = [
        load(tiles_hbm, tiles, 0),
        load(weight_hbm, weight_t, 1),
        load(cols_hbm, cols_ref, 2),
        load(cols_hbm, cols_held, 3),
    ]
    for copy in [load_degree, load_features, load_embeddings]:
        copy.start()

    barrier = pltpu.get_barrier_semaphore()

    quarter = n // 4
    head = me < 2 * quarter
    third = jnp.logical_and(me >= 2 * quarter, me < 3 * quarter)
    tail = me >= 3 * quarter

    def greet(to, carry):
        @pl.when(to != me)
        def _():
            pl.semaphore_signal(barrier, inc=1, device_id=(to,), device_id_type=MESH)

        return carry

    lax.fori_loop(jnp.where(tail, 2 * quarter, 0), n, greet, 0)
    for copy in small:
        copy.start()

    @pl.when(me == 0)
    def _():
        for i in range(pairs):
            exts[i][blocks : blocks + send_most] = jnp.zeros((send_most,) + exts[i].shape[1:], jnp.bfloat16)

    @pl.when(me == n - 1)
    def _():
        for i in range(pairs):
            exts[i][blocks + send_most :] = jnp.zeros((send_most,) + exts[i].shape[1:], jnp.bfloat16)

    load_degree.wait()
    roots = lax.rsqrt(degree[...].astype(jnp.float32)).T
    for b in range(blocks):
        inv[b] = jnp.broadcast_to(roots[:, b : b + 1], (tile, LANES))

    def rim_copy(i, side):
        first = blocks if side == 1 else blocks + send_most
        to = me + 1 if side == 1 else me - 1
        return pltpu.make_async_remote_copy(
            src_ref=sends[i].at[side],
            dst_ref=exts[i].at[pl.ds(first, send_most)],
            send_sem=send_sem.at[i % chunks],
            recv_sem=recv_sem.at[i % (2 * chunks)],
            device_id=(to,),
            device_id_type=MESH,
        )

    even = lax.rem(me, 2) == 0
    inner = jnp.logical_and(me > 0, me < n - 1)

    def wait_for(units, sem):
        some = counted.at[pl.ds(0, units)]
        pltpu.make_async_copy(some, some, sem).wait()

    def joint_wait(hub_rows, sem):
        @pl.when(inner)
        def _():
            wait_for(hub_rows + 2 * rim_units, sem)

        @pl.when(jnp.logical_not(inner))
        def _():
            wait_for(hub_rows + rim_units, sem)

    def hub_copy(i, held, owner, to, sem):
        return pltpu.make_async_remote_copy(
            src_ref=held,
            dst_ref=hub_bufs[i].at[owner],
            send_sem=send_sem.at[i % chunks],
            recv_sem=sem,
            device_id=(to,),
            device_id_type=MESH,
        )

    def row_of(rows, row):
        here = lax.broadcasted_iota(jnp.int32, rows.shape, 0) == lax.rem(row, 16)
        return jnp.sum(jnp.where(here, rows.astype(jnp.float32), 0.0), axis=0, keepdims=True)

    def stage_rims(i):
        for side in range(2):
            for s in range(send_most):
                block = locals_[i][listed_ref[0, side, s]]
                keep = jnp.where(s < count_ref[0, side], 1.0, 0.0).astype(jnp.float32)
                sends[i][side, s] = (block.astype(jnp.float32) * keep).astype(jnp.bfloat16)

    def stage_hubs(i):
        near = [groups[i][lax.div(hubs_ref[q], 16)] for q in range(hub_dev)]
        picked = [row_of(near[q], hubs_ref[q]) for q in range(hub_dev)]
        packed = jnp.concatenate(picked, axis=0).astype(jnp.bfloat16)
        hub_sends[i][...] = packed
        hub_bufs[i][me] = packed

    def launch_rims(i):
        @pl.when(even)
        def _():
            rim_copy(i, 1).start()

        @pl.when(me > 0)
        def _():
            rim_copy(i, 0).start()

        @pl.when(jnp.logical_and(jnp.logical_not(even), me < n - 1))
        def _():
            rim_copy(i, 1).start()

    def launch_hubs(i):
        joint = recv_sem.at[i % (2 * chunks)]

        def spread(step, carry):
            hub_copy(i, hub_sends[i], me, lax.rem(me + step, n), joint).start()
            return carry

        lax.fori_loop(1, n, spread, 0)

    def launch_first(c):
        joint = recv_sem.at[c]

        def spread(step, carry):
            hub_copy(c, hub_sends[c], me, lax.rem(me + step, n), joint).start()
            return carry

        @pl.when(head)
        def _():
            source = lax.div(me, quarter)
            passer = me + (2 - source) * quarter
            hub_copy(c, hub_sends[c], me, passer, pass_sem.at[c, source]).start()

            def near(step, carry):
                to = lax.rem(me + step, 3 * quarter)

                @pl.when(to != passer)
                def _():
                    hub_copy(c, hub_sends[c], me, to, joint).start()

                return carry

            lax.fori_loop(1, 3 * quarter, near, 0)

        @pl.when(jnp.logical_not(head))
        def _():
            lax.fori_loop(1, n, spread, 0)

    def pass_on(c, source):
        owner = me - (2 - source) * quarter
        wait_for(1, pass_sem.at[c, source])

        def spread(step, carry):
            to = 3 * quarter + lax.rem(me + step, quarter)
            hub_copy(c, hub_bufs[c].at[owner], owner, to, recv_sem.at[c]).start()
            return carry

        lax.fori_loop(0, quarter, spread, 0)

    def first_wait(sem, of_head, of_third):
        for group, hub_rows in ((head, of_head), (third, of_third), (tail, n - 1)):

            @pl.when(group)
            def _(hub_rows=hub_rows):
                joint_wait(hub_rows, sem)

    def prepare(c):
        which, at, width = pieces[c]

        def one(b, carry):
            rows = pl.ds(pl.multiple_of(b * tile, tile), tile)
            x = (features, embeddings)[which][rows, at : at + width]
            z = (x.astype(jnp.float32) * wide(inv[b], width)).astype(jnp.bfloat16)
            locals_[c][b] = z
            groups[c][pl.ds(b * per, per)] = z.reshape(per, 16, width)
            exts[c][b] = z
            return carry

        lax.fori_loop(0, blocks, one, 0, unroll=UNROLL)

    for copy in small + [load_features, load_embeddings]:
        copy.wait()
    for copy in late:
        copy.start()

    for c in range(chunks):
        with jax.named_scope("prepare"):
            prepare(c)
            stage_hubs(c)
            stage_rims(c)
        if c == 0:
            with jax.named_scope("barrier"):
                pl.semaphore_wait(barrier, n - 1 - jnp.where(head, quarter, 0))
        with jax.named_scope("launch"):
            launch_first(c)
            launch_rims(c)
    with jax.named_scope("weights"):
        for copy in late:
            copy.wait()
        weight[...] = weight_t[...].T

    @pl.when(third)
    def _():
        with jax.named_scope("pass"):
            for c in range(chunks):
                pass_on(c, 1)
                pass_on(c, 0)

    for hop in range(HOPS):
        for c in range(chunks):
            i = hop * chunks + c
            j = i + chunks
            which, at, width = pieces[c]
            with jax.named_scope(f"hubwait_{hop}_{c}"):
                if hop:
                    joint_wait(n - 1, recv_sem.at[i % (2 * chunks)])
                else:
                    first_wait(recv_sem.at[c], n - 1, n - 3)
            if i == pairs - 1:
                continue

            hubs = hub_bufs[i][...].reshape(n * hub_dev, width)

            def one(b, carry):
                rows = pl.ds(pl.multiple_of(b * tile, tile), tile)
                y = gathered(b, rows, taps, tiles, weight, cols_ref, exts[i], hubs)
                root = wide(inv[b], width)
                x = (y * root).astype(jnp.bfloat16)
                (out_f, out_e)[which][hop, rows, at : at + width] = x
                if hop + 1 < HOPS:
                    z = (x.astype(jnp.float32) * root).astype(jnp.bfloat16)
                    locals_[j][b] = z
                    groups[j][pl.ds(b * per, per)] = z.reshape(per, 16, width)
                    exts[j][b] = z
                return carry

            with jax.named_scope(f"compute_{hop}_{c}"):
                lax.fori_loop(0, blocks, one, 0, unroll=UNROLL)
            if hop + 1 < HOPS:
                with jax.named_scope(f"launch_{hop}_{c}"):
                    stage_hubs(j)
                    if hop:
                        joint_wait(n - 1, send_sem.at[c])
                    else:
                        first_wait(send_sem.at[c], n - 1 - quarter, n - 1 + 2 * quarter)
                    launch_hubs(j)
                    stage_rims(j)
                    launch_rims(j)

    with jax.named_scope("drain"):
        for i in range(pairs - chunks, pairs):
            joint_wait(n - 1, send_sem.at[i % chunks])


def flush(
    n, sizes, held_f, held_e, tiles, weight, inv, ext, hubs_ref, cols_held,
    out_f, out_e, cols, held, sem,
):
    blocks, tile, taps, send_most, hub_dev, pieces = sizes
    _, at, width = pieces[-1]
    last = HOPS - 1
    fetch = pltpu.make_async_copy(cols_held, cols, sem.at[0])
    fetch.start()
    copies = [
        pltpu.make_async_copy(held_f, out_f, sem.at[1]),
        pltpu.make_async_copy(held_e.at[:last], out_e.at[:last], sem.at[2]),
    ]
    if at:
        done = pl.ds(0, at)
        copies.append(pltpu.make_async_copy(held_e.at[last, :, done], out_e.at[last, :, done], sem.at[3]))
    for copy in copies:
        copy.start()
    fetch.wait()
    hubs = hubs_ref[...].reshape(n * hub_dev, width)

    def one(b, carry):
        rows = pl.ds(pl.multiple_of(b * tile, tile), tile)
        y = gathered(b, rows, taps, tiles, weight, cols, ext, hubs)
        held[rows, :] = (y * wide(inv[b], width)).astype(jnp.bfloat16)
        return carry

    lax.fori_loop(0, blocks, one, 0, unroll=UNROLL)
    rest = pltpu.make_async_copy(held, out_e.at[last, :, pl.ds(at, width)], sem.at[4])
    rest.start()
    for copy in copies + [rest]:
        copy.wait()


def body(
    features, embeddings, tile_values, tile_columns, send_blocks, send_count,
    hub_rows, hub_weight, degree,
):
    n = lax.axis_size("dom")
    rows = features.shape[0]
    blocks, taps, tile, _ = tile_values.shape
    send_most = send_blocks.shape[2]
    hub_dev = hub_rows.shape[0]
    pieces = cut(0, features.shape[1]) + cut(1, embeddings.shape[1])
    sizes = (blocks, tile, taps, send_most, hub_dev, pieces)
    widths = [width for _, _, width in pieces] * HOPS
    assert set(widths) == {WIDTH}
    units = 2 * send_most * tile // hub_dev
    vmem = pl.BlockSpec(memory_space=pltpu.VMEM)
    hbm = pl.BlockSpec(memory_space=pltpu.HBM)
    bf16 = jnp.bfloat16
    results = [
        ((HOPS, rows, features.shape[1]), bf16),
        ((HOPS, rows, embeddings.shape[1]), bf16),
        (tile_values.shape, bf16),
        ((rows, n * hub_dev), bf16),
        ((blocks, tile, LANES), jnp.float32),
        ((blocks + 2 * send_most, tile, widths[-1]), bf16),
        ((n, hub_dev, widths[-1]), bf16),
        ((taps, blocks), jnp.int32),
    ]
    out_bytes = sum(math.prod(shape[:-1]) * max(shape[-1], LANES) * jnp.dtype(kind).itemsize for shape, kind in results)
    held = pl.pallas_call(
        functools.partial(kernel, n, sizes),
        out_shape=tuple(pltpu.VMEM(shape, kind) for shape, kind in results),
        in_specs=[hbm] * 9,
        out_specs=(vmem,) * len(results),
        scratch_shapes=[pltpu.VMEM((n + n // 2 + units, hub_dev, WIDTH), bf16)]
        + [
            pltpu.VMEM(shape + (width,), bf16)
            for shape, some in (
                ((blocks, tile), widths),
                ((rows // 16, 16), widths),
                ((2, send_most, tile), widths),
                ((hub_dev,), widths),
                ((blocks + 2 * send_most, tile), widths[:-1]),
                ((n, hub_dev), widths[:-1]),
            )
            for width in some
        ]
        + [
            pltpu.SMEM((taps, blocks), jnp.int32),
            pltpu.SMEM(send_blocks.shape, jnp.int32),
            pltpu.SMEM(send_count.shape, jnp.int32),
            pltpu.SMEM(hub_rows.shape, jnp.int32),
            pltpu.VMEM(features.shape, bf16),
            pltpu.VMEM(embeddings.shape, bf16),
            pltpu.VMEM((n * hub_dev, rows), bf16),
            pltpu.VMEM((blocks, tile), jnp.int32),
            pltpu.SemaphoreType.DMA((6,)),
            pltpu.SemaphoreType.DMA((len(pieces),)),
            pltpu.SemaphoreType.DMA((2 * len(pieces),)),
            pltpu.SemaphoreType.DMA((len(pieces), 2)),
        ],
        compiler_params=pltpu.CompilerParams(
            collective_id=0, has_side_effects=True, vmem_limit_bytes=VMEM - out_bytes - 2**20
        ),
    )(
        tile_columns.T, send_blocks, send_count, hub_rows,
        features, embeddings, tile_values, hub_weight.T,
        degree.reshape(blocks, tile),
    )
    return pl.pallas_call(
        functools.partial(flush, n, sizes),
        out_shape=tuple(jax.ShapeDtypeStruct(h.shape, h.dtype) for h in held[:2]),
        in_specs=[vmem] * len(held),
        out_specs=(hbm, hbm),
        scratch_shapes=[
            pltpu.SMEM((taps, blocks), jnp.int32),
            pltpu.VMEM((rows, widths[-1]), bf16),
            pltpu.SemaphoreType.DMA((5,)),
        ],
        compiler_params=pltpu.CompilerParams(vmem_limit_bytes=4 * 2**20),
    )(*held)


def solution(mesh):
    placed = (
        P("dom", None),
        P("dom", None),
        P("dom", None, None, None),
        P("dom", None),
        P("dom", None, None),
        P("dom", None),
        P("dom"),
        P("dom", None),
        P("dom"),
    )
    return jax.shard_map(
        body,
        mesh=mesh,
        in_specs=placed,
        out_specs=(P(None, "dom", None), P(None, "dom", None)),
        check_vma=False,
    )
```

```python
import functools
import math

import jax
import jax.numpy as jnp
from jax import lax
from jax.experimental import pallas as pl
from jax.experimental.pallas import tpu as pltpu
from jax.sharding import PartitionSpec as P

HOPS = 3
LANES = 128
WIDTH = 128
UNROLL = 4
VMEM = 67043328
MESH = pl.DeviceIdType.MESH


def cut(which, columns):
    return [(which, at, min(WIDTH, columns - at)) for at in range(0, columns, WIDTH)]


def wide(root, width):
    return jnp.concatenate([root] * (width // LANES), axis=1)


def gathered(b, rows, taps, tiles, weight, cols, ext, hubs):
    left = jnp.concatenate([tiles[b, k] for k in range(taps)], axis=1)
    right = jnp.concatenate([ext[cols[k, b]] for k in range(taps)], axis=0)
    y = jnp.dot(left, right, preferred_element_type=jnp.float32)
    return y + jnp.dot(weight[rows, :], hubs, preferred_element_type=jnp.float32)


def kernel(
    n, sizes, cols_hbm, listed_hbm, count_hbm, hubs_hbm,
    features_hbm, embeddings_hbm, tiles_hbm, weight_hbm, degree_hbm,
    out_f, out_e, tiles, weight, inv, last_ext, last_hubs, cols_held, *scratch,
):
    blocks, tile, taps, send_most, hub_dev, pieces = sizes
    chunks = len(pieces)
    per = tile // 16
    pairs = HOPS * chunks
    scratch = list(scratch)
    counted = scratch.pop(0)
    rim_units = send_most * tile // hub_dev
    take = lambda count: [scratch.pop(0) for _ in range(count)]
    locals_, groups, sends, hub_sends = (take(pairs) for _ in range(4))
    exts = take(pairs - 1) + [last_ext]
    hub_bufs = take(pairs - 1) + [last_hubs]
    (
        cols_ref, listed_ref, count_ref, hubs_ref,
        features, embeddings, weight_t, degree,
        load_sem, send_sem, recv_sem, pass_sem,
    ) = scratch
    me = lax.axis_index("dom")

    def load(source, held, q):
        return pltpu.make_async_copy(source, held, load_sem.at[q])

    load_degree = load(degree_hbm, degree, 0)
    lead = pieces[0][2]
    rest = features.shape[1] - lead
    load_features = load(features_hbm.at[:, pl.ds(0, lead)], features.at[:, pl.ds(0, lead)], 1)
    load_rest = load(features_hbm.at[:, pl.ds(lead, rest)], features.at[:, pl.ds(lead, rest)], 6)
    load_embeddings = load(embeddings_hbm, embeddings, 2)
    small = [
        load(listed_hbm, listed_ref, 3),
        load(count_hbm, count_ref, 4),
        load(hubs_hbm, hubs_ref, 5),
    ]
    late = [
        load(tiles_hbm, tiles, 0),
        load(weight_hbm, weight_t, 1),
        load(cols_hbm, cols_ref, 2),
        load(cols_hbm, cols_held, 3),
    ]
    for copy in [load_degree, load_features, load_rest, load_embeddings]:
        copy.start()

    barrier = pltpu.get_barrier_semaphore()

    quarter = n // 4
    head = me < 2 * quarter
    third = jnp.logical_and(me >= 2 * quarter, me < 3 * quarter)
    tail = me >= 3 * quarter

    def greet(to, carry):
        @pl.when(to != me)
        def _():
            pl.semaphore_signal(barrier, inc=1, device_id=(to,), device_id_type=MESH)

        return carry

    lax.fori_loop(jnp.where(tail, 2 * quarter, 0), n, greet, 0)
    for copy in small:
        copy.start()

    @pl.when(me == 0)
    def _():
        for i in range(pairs):
            exts[i][blocks : blocks + send_most] = jnp.zeros((send_most,) + exts[i].shape[1:], jnp.bfloat16)

    @pl.when(me == n - 1)
    def _():
        for i in range(pairs):
            exts[i][blocks + send_most :] = jnp.zeros((send_most,) + exts[i].shape[1:], jnp.bfloat16)

    load_degree.wait()
    roots = lax.rsqrt(degree[...].astype(jnp.float32)).T
    for b in range(blocks):
        inv[b] = jnp.broadcast_to(roots[:, b : b + 1], (tile, LANES))

    def rim_copy(i, side):
        first = blocks if side == 1 else blocks + send_most
        to = me + 1 if side == 1 else me - 1
        return pltpu.make_async_remote_copy(
            src_ref=sends[i].at[side],
            dst_ref=exts[i].at[pl.ds(first, send_most)],
            send_sem=send_sem.at[i % chunks],
            recv_sem=recv_sem.at[i % (2 * chunks)],
            device_id=(to,),
            device_id_type=MESH,
        )

    even = lax.rem(me, 2) == 0
    inner = jnp.logical_and(me > 0, me < n - 1)

    def wait_for(units, sem):
        some = counted.at[pl.ds(0, units)]
        pltpu.make_async_copy(some, some, sem).wait()

    def joint_wait(hub_rows, sem):
        @pl.when(inner)
        def _():
            wait_for(hub_rows + 2 * rim_units, sem)

        @pl.when(jnp.logical_not(inner))
        def _():
            wait_for(hub_rows + rim_units, sem)

    def hub_copy(i, held, owner, to, sem):
        return pltpu.make_async_remote_copy(
            src_ref=held,
            dst_ref=hub_bufs[i].at[owner],
            send_sem=send_sem.at[i % chunks],
            recv_sem=sem,
            device_id=(to,),
            device_id_type=MESH,
        )

    def row_of(rows, row):
        here = lax.broadcasted_iota(jnp.int32, rows.shape, 0) == lax.rem(row, 16)
        return jnp.sum(jnp.where(here, rows.astype(jnp.float32), 0.0), axis=0, keepdims=True)

    def stage_rims(i):
        for side in range(2):
            for s in range(send_most):
                block = locals_[i][listed_ref[0, side, s]]
                keep = jnp.where(s < count_ref[0, side], 1.0, 0.0).astype(jnp.float32)
                sends[i][side, s] = (block.astype(jnp.float32) * keep).astype(jnp.bfloat16)

    def stage_hubs(i):
        near = [groups[i][lax.div(hubs_ref[q], 16)] for q in range(hub_dev)]
        picked = [row_of(near[q], hubs_ref[q]) for q in range(hub_dev)]
        packed = jnp.concatenate(picked, axis=0).astype(jnp.bfloat16)
        hub_sends[i][...] = packed
        hub_bufs[i][me] = packed

    def launch_rims(i):
        @pl.when(even)
        def _():
            rim_copy(i, 1).start()

        @pl.when(me > 0)
        def _():
            rim_copy(i, 0).start()

        @pl.when(jnp.logical_and(jnp.logical_not(even), me < n - 1))
        def _():
            rim_copy(i, 1).start()

    def launch_hubs(i):
        joint = recv_sem.at[i % (2 * chunks)]

        def spread(step, carry):
            hub_copy(i, hub_sends[i], me, lax.rem(me + step, n), joint).start()
            return carry

        lax.fori_loop(1, n, spread, 0)

    def launch_first(c):
        joint = recv_sem.at[c]

        def spread(step, carry):
            hub_copy(c, hub_sends[c], me, lax.rem(me + step, n), joint).start()
            return carry

        @pl.when(head)
        def _():
            source = lax.div(me, quarter)
            passer = me + (2 - source) * quarter
            hub_copy(c, hub_sends[c], me, passer, pass_sem.at[c, source]).start()

            def near(step, carry):
                to = lax.rem(me + step, 3 * quarter)

                @pl.when(to != passer)
                def _():
                    hub_copy(c, hub_sends[c], me, to, joint).start()

                return carry

            lax.fori_loop(1, 3 * quarter, near, 0)

        @pl.when(jnp.logical_not(head))
        def _():
            lax.fori_loop(1, n, spread, 0)

    def pass_on(c, source):
        owner = me - (2 - source) * quarter
        wait_for(1, pass_sem.at[c, source])

        def spread(step, carry):
            to = 3 * quarter + lax.rem(me + step, quarter)
            hub_copy(c, hub_bufs[c].at[owner], owner, to, recv_sem.at[c]).start()
            return carry

        lax.fori_loop(0, quarter, spread, 0)

    def first_wait(sem, of_head, of_third):
        for group, hub_rows in ((head, of_head), (third, of_third), (tail, n - 1)):

            @pl.when(group)
            def _(hub_rows=hub_rows):
                joint_wait(hub_rows, sem)

    def prepare(c):
        which, at, width = pieces[c]

        def one(b, carry):
            rows = pl.ds(pl.multiple_of(b * tile, tile), tile)
            x = (features, embeddings)[which][rows, at : at + width]
            z = (x.astype(jnp.float32) * wide(inv[b], width)).astype(jnp.bfloat16)
            locals_[c][b] = z
            groups[c][pl.ds(b * per, per)] = z.reshape(per, 16, width)
            exts[c][b] = z
            return carry

        lax.fori_loop(0, blocks, one, 0, unroll=UNROLL)

    for copy in small + [load_features]:
        copy.wait()

    for c in range(chunks):
        if c == 1:
            load_rest.wait()
            load_embeddings.wait()
            for copy in late:
                copy.start()
        with jax.named_scope("prepare"):
            prepare(c)
            stage_hubs(c)
            stage_rims(c)
        if c == 0:
            with jax.named_scope("barrier"):
                pl.semaphore_wait(barrier, n - 1 - jnp.where(head, quarter, 0))
        with jax.named_scope("launch"):
            launch_first(c)
            launch_rims(c)
    with jax.named_scope("weights"):
        for copy in late:
            copy.wait()
        weight[...] = weight_t[...].T

    @pl.when(third)
    def _():
        with jax.named_scope("pass"):
            for c in range(chunks):
                pass_on(c, 1)
                pass_on(c, 0)

    for hop in range(HOPS):
        for c in range(chunks):
            i = hop * chunks + c
            j = i + chunks
            which, at, width = pieces[c]
            with jax.named_scope(f"hubwait_{hop}_{c}"):
                if hop:
                    joint_wait(n - 1, recv_sem.at[i % (2 * chunks)])
                else:
                    first_wait(recv_sem.at[c], n - 1, n - 3)
            if i == pairs - 1:
                continue

            hubs = hub_bufs[i][...].reshape(n * hub_dev, width)

            def one(b, carry):
                rows = pl.ds(pl.multiple_of(b * tile, tile), tile)
                y = gathered(b, rows, taps, tiles, weight, cols_ref, exts[i], hubs)
                root = wide(inv[b], width)
                x = (y * root).astype(jnp.bfloat16)
                (out_f, out_e)[which][hop, rows, at : at + width] = x
                if hop + 1 < HOPS:
                    z = (x.astype(jnp.float32) * root).astype(jnp.bfloat16)
                    locals_[j][b] = z
                    groups[j][pl.ds(b * per, per)] = z.reshape(per, 16, width)
                    exts[j][b] = z
                return carry

            with jax.named_scope(f"compute_{hop}_{c}"):
                lax.fori_loop(0, blocks, one, 0, unroll=UNROLL)
            if hop + 1 < HOPS:
                with jax.named_scope(f"launch_{hop}_{c}"):
                    stage_hubs(j)
                    if hop:
                        joint_wait(n - 1, send_sem.at[c])
                    else:
                        first_wait(send_sem.at[c], n - 1 - quarter, n - 1 + 2 * quarter)
                    launch_hubs(j)
                    stage_rims(j)
                    launch_rims(j)

    with jax.named_scope("drain"):
        for i in range(pairs - chunks, pairs):
            joint_wait(n - 1, send_sem.at[i % chunks])


def flush(
    n, sizes, held_f, held_e, tiles, weight, inv, ext, hubs_ref, cols_held,
    out_f, out_e, cols, held, sem,
):
    blocks, tile, taps, send_most, hub_dev, pieces = sizes
    _, at, width = pieces[-1]
    last = HOPS - 1
    fetch = pltpu.make_async_copy(cols_held, cols, sem.at[0])
    fetch.start()
    copies = [
        pltpu.make_async_copy(held_f, out_f, sem.at[1]),
        pltpu.make_async_copy(held_e.at[:last], out_e.at[:last], sem.at[2]),
    ]
    if at:
        done = pl.ds(0, at)
        copies.append(pltpu.make_async_copy(held_e.at[last, :, done], out_e.at[last, :, done], sem.at[3]))
    for copy in copies:
        copy.start()
    fetch.wait()
    hubs = hubs_ref[...].reshape(n * hub_dev, width)

    def one(b, carry):
        rows = pl.ds(pl.multiple_of(b * tile, tile), tile)
        y = gathered(b, rows, taps, tiles, weight, cols, ext, hubs)
        held[rows, :] = (y * wide(inv[b], width)).astype(jnp.bfloat16)
        return carry

    lax.fori_loop(0, blocks, one, 0, unroll=UNROLL)
    rest = pltpu.make_async_copy(held, out_e.at[last, :, pl.ds(at, width)], sem.at[4])
    rest.start()
    for copy in copies + [rest]:
        copy.wait()


def body(
    features, embeddings, tile_values, tile_columns, send_blocks, send_count,
    hub_rows, hub_weight, degree,
):
    n = lax.axis_size("dom")
    rows = features.shape[0]
    blocks, taps, tile, _ = tile_values.shape
    send_most = send_blocks.shape[2]
    hub_dev = hub_rows.shape[0]
    pieces = cut(0, features.shape[1]) + cut(1, embeddings.shape[1])
    sizes = (blocks, tile, taps, send_most, hub_dev, pieces)
    widths = [width for _, _, width in pieces] * HOPS
    assert set(widths) == {WIDTH}
    units = 2 * send_most * tile // hub_dev
    vmem = pl.BlockSpec(memory_space=pltpu.VMEM)
    hbm = pl.BlockSpec(memory_space=pltpu.HBM)
    bf16 = jnp.bfloat16
    results = [
        ((HOPS, rows, features.shape[1]), bf16),
        ((HOPS, rows, embeddings.shape[1]), bf16),
        (tile_values.shape, bf16),
        ((rows, n * hub_dev), bf16),
        ((blocks, tile, LANES), jnp.float32),
        ((blocks + 2 * send_most, tile, widths[-1]), bf16),
        ((n, hub_dev, widths[-1]), bf16),
        ((taps, blocks), jnp.int32),
    ]
    out_bytes = sum(math.prod(shape[:-1]) * max(shape[-1], LANES) * jnp.dtype(kind).itemsize for shape, kind in results)
    held = pl.pallas_call(
        functools.partial(kernel, n, sizes),
        out_shape=tuple(pltpu.VMEM(shape, kind) for shape, kind in results),
        in_specs=[hbm] * 9,
        out_specs=(vmem,) * len(results),
        scratch_shapes=[pltpu.VMEM((n + n // 2 + units, hub_dev, WIDTH), bf16)]
        + [
            pltpu.VMEM(shape + (width,), bf16)
            for shape, some in (
                ((blocks, tile), widths),
                ((rows // 16, 16), widths),
                ((2, send_most, tile), widths),
                ((hub_dev,), widths),
                ((blocks + 2 * send_most, tile), widths[:-1]),
                ((n, hub_dev), widths[:-1]),
            )
            for width in some
        ]
        + [
            pltpu.SMEM((taps, blocks), jnp.int32),
            pltpu.SMEM(send_blocks.shape, jnp.int32),
            pltpu.SMEM(send_count.shape, jnp.int32),
            pltpu.SMEM(hub_rows.shape, jnp.int32),
            pltpu.VMEM(features.shape, bf16),
            pltpu.VMEM(embeddings.shape, bf16),
            pltpu.VMEM((n * hub_dev, rows), bf16),
            pltpu.VMEM((blocks, tile), jnp.int32),
            pltpu.SemaphoreType.DMA((7,)),
            pltpu.SemaphoreType.DMA((len(pieces),)),
            pltpu.SemaphoreType.DMA((2 * len(pieces),)),
            pltpu.SemaphoreType.DMA((len(pieces), 2)),
        ],
        compiler_params=pltpu.CompilerParams(
            collective_id=0, has_side_effects=True, vmem_limit_bytes=VMEM - out_bytes - 2**20
        ),
    )(
        tile_columns.T, send_blocks, send_count, hub_rows,
        features, embeddings, tile_values, hub_weight.T,
        degree.reshape(blocks, tile),
    )
    return pl.pallas_call(
        functools.partial(flush, n, sizes),
        out_shape=tuple(jax.ShapeDtypeStruct(h.shape, h.dtype) for h in held[:2]),
        in_specs=[vmem] * len(held),
        out_specs=(hbm, hbm),
        scratch_shapes=[
            pltpu.SMEM((taps, blocks), jnp.int32),
            pltpu.VMEM((rows, widths[-1]), bf16),
            pltpu.SemaphoreType.DMA((5,)),
        ],
        compiler_params=pltpu.CompilerParams(vmem_limit_bytes=4 * 2**20),
    )(*held)


def solution(mesh):
    placed = (
        P("dom", None),
        P("dom", None),
        P("dom", None, None, None),
        P("dom", None),
        P("dom", None, None),
        P("dom", None),
        P("dom"),
        P("dom", None),
        P("dom"),
    )
    return jax.shard_map(
        body,
        mesh=mesh,
        in_specs=placed,
        out_specs=(P(None, "dom", None), P(None, "dom", None)),
        check_vma=False,
    )
```

```python
import functools
import math

import jax
import jax.numpy as jnp
from jax import lax
from jax.experimental import pallas as pl
from jax.experimental.pallas import tpu as pltpu
from jax.sharding import PartitionSpec as P

HOPS = 3
LANES = 128
WIDTH = 128
UNROLL = 4
VMEM = 67043328
MESH = pl.DeviceIdType.MESH


def cut(which, columns):
    return [(which, at, min(WIDTH, columns - at)) for at in range(0, columns, WIDTH)]


def wide(root, width):
    return jnp.concatenate([root] * (width // LANES), axis=1)


def gathered(b, rows, taps, tiles, weight, cols, ext, hubs):
    left = jnp.concatenate([tiles[b, k] for k in range(taps)], axis=1)
    right = jnp.concatenate([ext[cols[k, b]] for k in range(taps)], axis=0)
    y = jnp.dot(left, right, preferred_element_type=jnp.float32)
    return y + jnp.dot(weight[rows, :], hubs, preferred_element_type=jnp.float32)


def kernel(
    n, sizes, cols_hbm, listed_hbm, count_hbm, hubs_hbm,
    features_hbm, embeddings_hbm, tiles_hbm, weight_hbm, degree_hbm,
    out_f, out_e, tiles, weight, inv, last_ext, last_hubs, cols_held, *scratch,
):
    blocks, tile, taps, send_most, hub_dev, pieces = sizes
    chunks = len(pieces)
    per = tile // 16
    pairs = HOPS * chunks
    scratch = list(scratch)
    counted = scratch.pop(0)
    rim_units = send_most * tile // hub_dev
    take = lambda count: [scratch.pop(0) for _ in range(count)]
    locals_, groups, sends, hub_sends = (take(pairs) for _ in range(4))
    exts = take(pairs - 1) + [last_ext]
    hub_bufs = take(pairs - 1) + [last_hubs]
    (
        cols_ref, listed_ref, count_ref, hubs_ref,
        features, embeddings, weight_t, degree,
        load_sem, send_sem, recv_sem, pass_sem,
    ) = scratch
    me = lax.axis_index("dom")

    def load(source, held, q):
        return pltpu.make_async_copy(source, held, load_sem.at[q])

    load_degree = load(degree_hbm, degree, 0)
    load_features = load(features_hbm, features, 1)
    load_embeddings = load(embeddings_hbm, embeddings, 2)
    small = [
        load(listed_hbm, listed_ref, 3),
        load(count_hbm, count_ref, 4),
        load(hubs_hbm, hubs_ref, 5),
    ]
    late = [
        load(tiles_hbm, tiles, 0),
        load(weight_hbm, weight_t, 1),
        load(cols_hbm, cols_ref, 2),
        load(cols_hbm, cols_held, 3),
    ]
    for copy in [load_degree, load_features, load_embeddings]:
        copy.start()

    barrier = pltpu.get_barrier_semaphore()

    quarter = n // 4
    head = me < 2 * quarter
    third = jnp.logical_and(me >= 2 * quarter, me < 3 * quarter)
    tail = me >= 3 * quarter

    def greet(to, carry):
        @pl.when(to != me)
        def _():
            pl.semaphore_signal(barrier, inc=1, device_id=(to,), device_id_type=MESH)

        return carry

    lax.fori_loop(jnp.where(tail, 2 * quarter, 0), n, greet, 0)
    for copy in small:
        copy.start()

    @pl.when(me == 0)
    def _():
        for i in range(pairs):
            exts[i][blocks : blocks + send_most] = jnp.zeros((send_most,) + exts[i].shape[1:], jnp.bfloat16)

    @pl.when(me == n - 1)
    def _():
        for i in range(pairs):
            exts[i][blocks + send_most :] = jnp.zeros((send_most,) + exts[i].shape[1:], jnp.bfloat16)

    load_degree.wait()
    roots = lax.rsqrt(degree[...].astype(jnp.float32)).T
    for b in range(blocks):
        inv[b] = jnp.broadcast_to(roots[:, b : b + 1], (tile, LANES))

    def rim_copy(i, side):
        first = blocks if side == 1 else blocks + send_most
        to = me + 1 if side == 1 else me - 1
        return pltpu.make_async_remote_copy(
            src_ref=sends[i].at[side],
            dst_ref=exts[i].at[pl.ds(first, send_most)],
            send_sem=send_sem.at[i % chunks],
            recv_sem=recv_sem.at[i % (2 * chunks)],
            device_id=(to,),
            device_id_type=MESH,
        )

    even = lax.rem(me, 2) == 0
    inner = jnp.logical_and(me > 0, me < n - 1)

    def wait_for(units, sem):
        some = counted.at[pl.ds(0, units)]
        pltpu.make_async_copy(some, some, sem).wait()

    def joint_wait(hub_rows, sem):
        @pl.when(inner)
        def _():
            wait_for(hub_rows + 2 * rim_units, sem)

        @pl.when(jnp.logical_not(inner))
        def _():
            wait_for(hub_rows + rim_units, sem)

    def hub_copy(i, held, owner, to, sem):
        return pltpu.make_async_remote_copy(
            src_ref=held,
            dst_ref=hub_bufs[i].at[owner],
            send_sem=send_sem.at[i % chunks],
            recv_sem=sem,
            device_id=(to,),
            device_id_type=MESH,
        )

    def row_of(rows, row):
        here = lax.broadcasted_iota(jnp.int32, rows.shape, 0) == lax.rem(row, 16)
        return jnp.sum(jnp.where(here, rows.astype(jnp.float32), 0.0), axis=0, keepdims=True)

    def stage_rims(i):
        for side in range(2):
            for s in range(send_most):
                block = locals_[i][listed_ref[0, side, s]]
                keep = jnp.where(s < count_ref[0, side], 1.0, 0.0).astype(jnp.float32)
                sends[i][side, s] = (block.astype(jnp.float32) * keep).astype(jnp.bfloat16)

    def stage_hubs(i):
        near = [groups[i][lax.div(hubs_ref[q], 16)] for q in range(hub_dev)]
        picked = [row_of(near[q], hubs_ref[q]) for q in range(hub_dev)]
        packed = jnp.concatenate(picked, axis=0).astype(jnp.bfloat16)
        hub_sends[i][...] = packed
        hub_bufs[i][me] = packed

    def launch_rims(i):
        @pl.when(even)
        def _():
            rim_copy(i, 1).start()

        @pl.when(me > 0)
        def _():
            rim_copy(i, 0).start()

        @pl.when(jnp.logical_and(jnp.logical_not(even), me < n - 1))
        def _():
            rim_copy(i, 1).start()

    def launch_hubs(i):
        joint = recv_sem.at[i % (2 * chunks)]

        def spread(step, carry):
            hub_copy(i, hub_sends[i], me, step + (step >= me).astype(jnp.int32), joint).start()
            return carry

        lax.fori_loop(0, n - 1, spread, 0)

    def launch_first(c):
        joint = recv_sem.at[c]

        def spread(step, carry):
            hub_copy(c, hub_sends[c], me, lax.rem(me + step, n), joint).start()
            return carry

        @pl.when(head)
        def _():
            source = lax.div(me, quarter)
            passer = me + (2 - source) * quarter
            hub_copy(c, hub_sends[c], me, passer, pass_sem.at[c, source]).start()

            def near(step, carry):
                to = lax.rem(me + step, 3 * quarter)

                @pl.when(to != passer)
                def _():
                    hub_copy(c, hub_sends[c], me, to, joint).start()

                return carry

            lax.fori_loop(1, 3 * quarter, near, 0)

        @pl.when(jnp.logical_not(head))
        def _():
            lax.fori_loop(1, n, spread, 0)

    def pass_on(c, source):
        owner = me - (2 - source) * quarter
        wait_for(1, pass_sem.at[c, source])

        def spread(step, carry):
            to = 3 * quarter + lax.rem(me + step, quarter)
            hub_copy(c, hub_bufs[c].at[owner], owner, to, recv_sem.at[c]).start()
            return carry

        lax.fori_loop(0, quarter, spread, 0)

    def first_wait(sem, of_head, of_third):
        for group, hub_rows in ((head, of_head), (third, of_third), (tail, n - 1)):

            @pl.when(group)
            def _(hub_rows=hub_rows):
                joint_wait(hub_rows, sem)

    def prepare(c):
        which, at, width = pieces[c]

        def one(b, carry):
            rows = pl.ds(pl.multiple_of(b * tile, tile), tile)
            x = (features, embeddings)[which][rows, at : at + width]
            z = (x.astype(jnp.float32) * wide(inv[b], width)).astype(jnp.bfloat16)
            locals_[c][b] = z
            groups[c][pl.ds(b * per, per)] = z.reshape(per, 16, width)
            exts[c][b] = z
            return carry

        lax.fori_loop(0, blocks, one, 0, unroll=UNROLL)

    for copy in small + [load_features, load_embeddings]:
        copy.wait()
    for copy in late:
        copy.start()

    for c in range(chunks):
        with jax.named_scope("prepare"):
            prepare(c)
            stage_hubs(c)
            stage_rims(c)
        if c == 0:
            with jax.named_scope("barrier"):
                pl.semaphore_wait(barrier, n - 1 - jnp.where(head, quarter, 0))
        with jax.named_scope("launch"):
            launch_first(c)
            launch_rims(c)
    with jax.named_scope("weights"):
        for copy in late:
            copy.wait()
        weight[...] = weight_t[...].T

    @pl.when(third)
    def _():
        with jax.named_scope("pass"):
            for c in range(chunks):
                pass_on(c, 1)
                pass_on(c, 0)

    for hop in range(HOPS):
        for c in range(chunks):
            i = hop * chunks + c
            j = i + chunks
            which, at, width = pieces[c]
            with jax.named_scope(f"hubwait_{hop}_{c}"):
                if hop:
                    joint_wait(n - 1, recv_sem.at[i % (2 * chunks)])
                else:
                    first_wait(recv_sem.at[c], n - 1, n - 3)
            if i == pairs - 1:
                continue

            hubs = hub_bufs[i][...].reshape(n * hub_dev, width)

            def one(b, carry):
                rows = pl.ds(pl.multiple_of(b * tile, tile), tile)
                y = gathered(b, rows, taps, tiles, weight, cols_ref, exts[i], hubs)
                root = wide(inv[b], width)
                x = (y * root).astype(jnp.bfloat16)
                (out_f, out_e)[which][hop, rows, at : at + width] = x
                if hop + 1 < HOPS:
                    z = (x.astype(jnp.float32) * root).astype(jnp.bfloat16)
                    locals_[j][b] = z
                    groups[j][pl.ds(b * per, per)] = z.reshape(per, 16, width)
                    exts[j][b] = z
                return carry

            with jax.named_scope(f"compute_{hop}_{c}"):
                lax.fori_loop(0, blocks, one, 0, unroll=UNROLL)
            if hop + 1 < HOPS:
                with jax.named_scope(f"launch_{hop}_{c}"):
                    stage_hubs(j)
                    if hop:
                        joint_wait(n - 1, send_sem.at[c])
                    else:
                        first_wait(send_sem.at[c], n - 1 - quarter, n - 1 + 2 * quarter)
                    launch_hubs(j)
                    stage_rims(j)
                    launch_rims(j)

    with jax.named_scope("drain"):
        for i in range(pairs - chunks, pairs):
            joint_wait(n - 1, send_sem.at[i % chunks])


def flush(
    n, sizes, held_f, held_e, tiles, weight, inv, ext, hubs_ref, cols_held,
    out_f, out_e, cols, held, sem,
):
    blocks, tile, taps, send_most, hub_dev, pieces = sizes
    _, at, width = pieces[-1]
    last = HOPS - 1
    fetch = pltpu.make_async_copy(cols_held, cols, sem.at[0])
    fetch.start()
    copies = [
        pltpu.make_async_copy(held_f, out_f, sem.at[1]),
        pltpu.make_async_copy(held_e.at[:last], out_e.at[:last], sem.at[2]),
    ]
    if at:
        done = pl.ds(0, at)
        copies.append(pltpu.make_async_copy(held_e.at[last, :, done], out_e.at[last, :, done], sem.at[3]))
    for copy in copies:
        copy.start()
    fetch.wait()
    hubs = hubs_ref[...].reshape(n * hub_dev, width)

    def one(b, carry):
        rows = pl.ds(pl.multiple_of(b * tile, tile), tile)
        y = gathered(b, rows, taps, tiles, weight, cols, ext, hubs)
        held[rows, :] = (y * wide(inv[b], width)).astype(jnp.bfloat16)
        return carry

    lax.fori_loop(0, blocks, one, 0, unroll=UNROLL)
    rest = pltpu.make_async_copy(held, out_e.at[last, :, pl.ds(at, width)], sem.at[4])
    rest.start()
    for copy in copies + [rest]:
        copy.wait()


def body(
    features, embeddings, tile_values, tile_columns, send_blocks, send_count,
    hub_rows, hub_weight, degree,
):
    n = lax.axis_size("dom")
    rows = features.shape[0]
    blocks, taps, tile, _ = tile_values.shape
    send_most = send_blocks.shape[2]
    hub_dev = hub_rows.shape[0]
    pieces = cut(0, features.shape[1]) + cut(1, embeddings.shape[1])
    sizes = (blocks, tile, taps, send_most, hub_dev, pieces)
    widths = [width for _, _, width in pieces] * HOPS
    assert set(widths) == {WIDTH}
    units = 2 * send_most * tile // hub_dev
    vmem = pl.BlockSpec(memory_space=pltpu.VMEM)
    hbm = pl.BlockSpec(memory_space=pltpu.HBM)
    bf16 = jnp.bfloat16
    results = [
        ((HOPS, rows, features.shape[1]), bf16),
        ((HOPS, rows, embeddings.shape[1]), bf16),
        (tile_values.shape, bf16),
        ((rows, n * hub_dev), bf16),
        ((blocks, tile, LANES), jnp.float32),
        ((blocks + 2 * send_most, tile, widths[-1]), bf16),
        ((n, hub_dev, widths[-1]), bf16),
        ((taps, blocks), jnp.int32),
    ]
    out_bytes = sum(math.prod(shape[:-1]) * max(shape[-1], LANES) * jnp.dtype(kind).itemsize for shape, kind in results)
    held = pl.pallas_call(
        functools.partial(kernel, n, sizes),
        out_shape=tuple(pltpu.VMEM(shape, kind) for shape, kind in results),
        in_specs=[hbm] * 9,
        out_specs=(vmem,) * len(results),
        scratch_shapes=[pltpu.VMEM((n + n // 2 + units, hub_dev, WIDTH), bf16)]
        + [
            pltpu.VMEM(shape + (width,), bf16)
            for shape, some in (
                ((blocks, tile), widths),
                ((rows // 16, 16), widths),
                ((2, send_most, tile), widths),
                ((hub_dev,), widths),
                ((blocks + 2 * send_most, tile), widths[:-1]),
                ((n, hub_dev), widths[:-1]),
            )
            for width in some
        ]
        + [
            pltpu.SMEM((taps, blocks), jnp.int32),
            pltpu.SMEM(send_blocks.shape, jnp.int32),
            pltpu.SMEM(send_count.shape, jnp.int32),
            pltpu.SMEM(hub_rows.shape, jnp.int32),
            pltpu.VMEM(features.shape, bf16),
            pltpu.VMEM(embeddings.shape, bf16),
            pltpu.VMEM((n * hub_dev, rows), bf16),
            pltpu.VMEM((blocks, tile), jnp.int32),
            pltpu.SemaphoreType.DMA((6,)),
            pltpu.SemaphoreType.DMA((len(pieces),)),
            pltpu.SemaphoreType.DMA((2 * len(pieces),)),
            pltpu.SemaphoreType.DMA((len(pieces), 2)),
        ],
        compiler_params=pltpu.CompilerParams(
            collective_id=0, has_side_effects=True, vmem_limit_bytes=VMEM - out_bytes - 2**20
        ),
    )(
        tile_columns.T, send_blocks, send_count, hub_rows,
        features, embeddings, tile_values, hub_weight.T,
        degree.reshape(blocks, tile),
    )
    return pl.pallas_call(
        functools.partial(flush, n, sizes),
        out_shape=tuple(jax.ShapeDtypeStruct(h.shape, h.dtype) for h in held[:2]),
        in_specs=[vmem] * len(held),
        out_specs=(hbm, hbm),
        scratch_shapes=[
            pltpu.SMEM((taps, blocks), jnp.int32),
            pltpu.VMEM((rows, widths[-1]), bf16),
            pltpu.SemaphoreType.DMA((5,)),
        ],
        compiler_params=pltpu.CompilerParams(vmem_limit_bytes=4 * 2**20),
    )(*held)


def solution(mesh):
    placed = (
        P("dom", None),
        P("dom", None),
        P("dom", None, None, None),
        P("dom", None),
        P("dom", None, None),
        P("dom", None),
        P("dom"),
        P("dom", None),
        P("dom"),
    )
    return jax.shard_map(
        body,
        mesh=mesh,
        in_specs=placed,
        out_specs=(P(None, "dom", None), P(None, "dom", None)),
        check_vma=False,
    )
```
